32 devices in a mesh: wide: 16 (over z, y, x), narrow: 2 (over core).
Axes of the slice: x: 2, y: 2, z: 4, core: 2. Of those that a mesh axis runs over, the one named last changes fastest.
Arguments:
- contributions: float32 [2, 3, 8192, 128], P('narrow', None, 'wide'), may hold values from -6 to 6
- send_map: int32 [16, 800], P('wide'), may hold values from -1 to 511, as said below
- arrival_map: int32 [16, 800], P('wide'), may hold values from -1 to 255, as said below
- dual_diagonal: float32 [4096, 128], P('wide'), may hold values from 0.5 to 2
- mortar: bfloat16 [4096, 128, 128], P('wide'), may hold values from -0.5 to 0.5
- master_inverse: bfloat16 [4096, 128, 128], P('wide'), may hold values from -0.5 to 0.5
Outputs:
- corrections: float32 [2, 3, 8192, 128], P('narrow', None, 'wide')
The draws below stay inside these ranges and needn't reach their ends.
Inputs may be any that keep to these rules, and one draw needn't show every extreme that they name: `send_map`: each row 0 to 511 of a partition stands in exactly one of its slots. Some stripe has all 50 of its slots used by every partition. arrival_map[d, o * 50 + c] is -1 exactly where send_map[o, d * 50 + c] is -1.
All inputs are finite; a program needn't handle non-finite values.
Results may differ from the reference program's by a relative error of at most 0.0041.
Values sent between devices are 32-bit elements; how exact they have to be, the bound alone decides.
A program may use at most 64 MiB of HBM per device.

```python
import math
import jax
import jax.numpy as jnp
from jax import lax

NODES = 128
COMP = 3
BLK_DEV = 256
BLOCKS = 4096
ROWS_OWN = 512
ROWS = 8192
CAP = 50
SLOTS = 800
N_WIDE = 16


def shared_maps(key):
    base = jax.random.fold_in(key, 7)
    key_hot, key_bias, key_jitter, key_tie, key_rows, key_block = jax.random.split(base, 6)
    hot_stripe = jax.random.randint(key_hot, (), 0, N_WIDE)
    stripe_bias = jax.random.randint(key_bias, (N_WIDE,), 0, 4)
    stripe_bias = stripe_bias * stripe_bias
    stripe_ids = jnp.arange(SLOTS, dtype=jnp.int32) // CAP
    random_perturbation = jax.random.randint(key_jitter, (N_WIDE, SLOTS), 0, 16)
    scores = jnp.where(stripe_ids[None, :] == hot_stripe, 1000, stripe_bias[stripe_ids][None, :] + random_perturbation)
    raw_ties = jax.random.randint(key_tie, (N_WIDE, SLOTS), 0, 1 << 30)
    tie_rank = jnp.argsort(jnp.argsort(raw_ties, axis=1), axis=1)
    priority_order = jnp.argsort(-(scores * SLOTS + tie_rank), axis=1)
    chosen = priority_order[:, :ROWS_OWN]
    row_order = jnp.argsort(jax.random.randint(key_rows, (N_WIDE, ROWS_OWN), 0, 1 << 30), axis=1).astype(jnp.int32)
    owners = jnp.arange(N_WIDE, dtype=jnp.int32)[:, None]
    send_map = jnp.full((N_WIDE, SLOTS), -1, jnp.int32).at[owners, chosen].set(row_order)
    by_stripe = jnp.transpose(send_map.reshape(N_WIDE, N_WIDE, CAP), (1, 0, 2)).reshape(N_WIDE, SLOTS)
    local_ids = jax.random.randint(key_block, (N_WIDE, SLOTS), 0, BLK_DEV)
    arrival_map = jnp.where(by_stripe >= 0, local_ids, -1).astype(jnp.int32)
    return (send_map, arrival_map)


def draw_send_map(key, part):
    return shared_maps(key)[0]


def draw_arrival_map(key, part):
    return shared_maps(key)[1]


def steps_of(key, shape, cuts, least, largest):
    def one(axis_at, shards_of):
        steps = jax.random.uniform(jax.random.fold_in(jax.random.fold_in(key, 6), axis_at), (shards_of,), jnp.float32, least / len(cuts), largest / len(cuts))
        return jnp.repeat(jnp.exp(steps), shape[axis_at] // shards_of).reshape((-1,) + (1,) * (len(shape) - axis_at - 1))

    level = one(*cuts[0])
    for cut in cuts[1:]:
        level = level * one(*cut)
    return level


def bell_draw(rng, shape, scale, most, cuts=(), kind=jnp.bfloat16):
    drawn = scale * jax.random.normal(rng, shape, jnp.float32)
    if cuts:
        drawn = drawn * steps_of(rng, shape, cuts, -0.22, 0.18)
    return jnp.clip(drawn, -most, most).astype(kind)


def setup_inputs(seed: int = 0) -> dict:
    seeds = jax.random.split(jax.random.key(seed), 7)
    return {
        "contributions": bell_draw(seeds[0], (2, COMP, ROWS, NODES), 1.0, 6.0, ((0, 2), (2, 16)), jnp.float32),
        "send_map": draw_send_map(jax.random.fold_in(seeds[6], 71), 0),
        "arrival_map": draw_arrival_map(jax.random.fold_in(seeds[6], 71), 0),
        "dual_diagonal": jnp.clip(jnp.exp(math.log(2.0) - 1.3862944 * jax.random.uniform(seeds[3], (BLOCKS, NODES), jnp.float32) ** steps_of(seeds[3], (BLOCKS, NODES), ((0, 16),), -0.2, 0.2)), 0.5, 2.0),
        "mortar": bell_draw(seeds[4], (BLOCKS, NODES, NODES), NODES ** -0.5, 0.5, ((0, 16),)),
        "master_inverse": bell_draw(seeds[5], (BLOCKS, NODES, NODES), NODES ** -0.5, 0.5, ((0, 16),)),
    }


def stripe_solve(pieces):
    summed, diagonal, mortar_part, inverse_part = pieces
    mortar_wide = mortar_part.astype(jnp.float32)
    inverse_wide = inverse_part.astype(jnp.float32)
    multiplier = summed[0] / diagonal[None]
    multiplier_low = lax.optimization_barrier(multiplier.astype(jnp.bfloat16)).astype(jnp.float32)
    pushed = jnp.einsum('bij,cbi->cbj', mortar_wide, multiplier_low, precision=lax.Precision.HIGHEST)
    condensed = summed[1] + pushed
    condensed_low = lax.optimization_barrier(condensed.astype(jnp.bfloat16)).astype(jnp.float32)
    master_fix = jnp.einsum('bkj,cbj->cbk', inverse_wide, condensed_low, precision=lax.Precision.HIGHEST)
    master_low = lax.optimization_barrier(master_fix.astype(jnp.bfloat16)).astype(jnp.float32)
    slave_fix = jnp.einsum('bij,cbj->cbi', mortar_wide, master_low, precision=lax.Precision.HIGHEST) / diagonal[None]
    return jnp.stack([slave_fix, master_fix])


def reference(contributions, send_map, arrival_map, dual_diagonal, mortar, master_inverse):
    owners = jnp.arange(N_WIDE, dtype=jnp.int32)[:, None]
    slot_ids = jnp.arange(SLOTS, dtype=jnp.int32)[None, :]
    stripes = slot_ids // CAP
    local_block = arrival_map[stripes, owners * CAP + slot_ids % CAP]
    is_live = send_map >= 0
    targets = jnp.where(is_live, owners * ROWS_OWN + send_map, ROWS).astype(jnp.int32)
    block_ids = (stripes * BLK_DEV + local_block).astype(jnp.int32)
    row_block = jnp.zeros((ROWS + 1,), jnp.int32).at[targets.reshape(-1)].set(block_ids.reshape(-1))[:ROWS]
    summed = jnp.zeros((2, COMP, BLOCKS, NODES), jnp.float32).at[:, :, row_block, :].add(contributions)
    by_stripe = jnp.transpose(summed.reshape(2, COMP, N_WIDE, BLK_DEV, NODES), (2, 0, 1, 3, 4))
    diag_parts = dual_diagonal.reshape(N_WIDE, BLK_DEV, NODES)
    mortar_parts = mortar.reshape(N_WIDE, BLK_DEV, NODES, NODES)
    inverse_parts = master_inverse.reshape(N_WIDE, BLK_DEV, NODES, NODES)
    fixes = lax.map(stripe_solve, (by_stripe, diag_parts, mortar_parts, inverse_parts))
    fixes = jnp.transpose(fixes, (1, 2, 0, 3, 4)).reshape(2, COMP, BLOCKS, NODES)
    return fixes[:, :, row_block, :]
```

```python
import functools

import jax
import jax.numpy as jnp
from jax import lax
from jax.experimental import pallas as pl
from jax.experimental.pallas import tpu as pltpu
from jax.sharding import PartitionSpec as P

GROUP = 16
SUBLANES = 8
LANES = 128
PLANES = 4
MESH = pl.DeviceIdType.MESH


def one_hot_dot(mask, values):
    high = values.astype(jnp.bfloat16)
    low = (values - high.astype(jnp.float32)).astype(jnp.bfloat16)
    return jnp.dot(mask, high, preferred_element_type=jnp.float32) + jnp.dot(
        mask, low, preferred_element_type=jnp.float32
    )


def block_products(vectors, matrices, transposed):
    rows = lax.broadcasted_iota(jnp.int32, vectors.shape, 0)
    total = jnp.zeros(vectors.shape, jnp.float32)
    for b in range(vectors.shape[0]):
        product = lax.dot_general(
            vectors,
            matrices(b),
            (((1,), (1 if transposed else 0,)), ((), ())),
            preferred_element_type=jnp.float32,
        )
        total = jnp.where(rows == b, product, total)
    return total


def kernel(
    n,
    cap,
    capp,
    contributions_hbm,
    send_hbm,
    arrival_hbm,
    diagonal_hbm,
    mortar_hbm,
    inverse_hbm,
    out,
    contributions,
    send_map,
    arrival_map,
    diagonal,
    mortar,
    inverse,
    send_row,
    own_row,
    far_row,
    hub_rows,
    pick_mask,
    place_mask,
    sum_mask,
    spread_mask,
    hub_sum_mask,
    hub_spread_mask,
    going,
    coming,
    hub_in,
    dense_out,
    dense_in,
    sums,
    pair,
    fix_pair,
    fixes,
    returning,
    up_in,
    relay,
    returned,
    load_sem,
    map_sem,
    fetch_sem,
    ids_send,
    ids_recv,
    own_send,
    own_recv,
    hub_send,
    hub_recv,
    dense_send,
    dense_recv,
    pair_send,
    pair_recv,
    back_send,
    back_recv,
    up_send,
    up_recv,
    ret_send,
    relay_send,
    ret_recv,
):
    me = lax.axis_index("wide")
    side = lax.axis_index("narrow")
    comps, row_count, nodes = out.shape[1:]
    m = n // 2
    p = n // PLANES
    slots = m * capp
    blocks = sums.shape[1]
    half = blocks // 2
    upper = me // m
    local = lax.rem(me, m)
    line = lax.rem(me, p)
    base = upper * m
    far_base = (1 - upper) * m
    my_hubs = (1 + upper) * p
    far_hub = (2 - upper) * p + line
    is_hub = me // p == 1 + upper
    is_outer = jnp.logical_not(is_hub)
    my_plane = local // p
    far_planes = (1 - upper, upper)
    mine = pl.multiple_of(side * half, half)
    theirs = pl.multiple_of((1 - side) * half, half)

    if capp > cap:
        first_pad = cap // SUBLANES * SUBLANES
        pad = pl.ds(first_pad, capp - first_pad)
        empty = jnp.zeros((comps, m, capp - first_pad, nodes), jnp.float32)
        coming[:, :, pad, :] = empty
        hub_in[:, 0, :, pad, :] = empty
        hub_in[:, 1, :, pad, :] = empty
        returned[:, 0:m, pad, :] = empty
        returned[:, m:n, pad, :] = empty

    barrier = pltpu.get_barrier_semaphore()

    def greet(device):
        pl.semaphore_signal(barrier, inc=1, device_id=device, device_id_type=MESH)

    def greet_half(k, carry):
        greet({"wide": base + lax.rem(local + k, m)})
        return carry

    lax.fori_loop(1, m, greet_half, 0)
    greet({"narrow": 1 - side})
    for s in range(2):
        greet({"wide": far_hub, "narrow": s})

    @pl.when(is_hub)
    def _():
        for s in range(2):
            for j in range(2):
                greet({"wide": far_base + j * p + line, "narrow": s})

    map_loads = [
        pltpu.make_async_copy(send_hbm, send_map, map_sem.at[0]),
        pltpu.make_async_copy(arrival_hbm, arrival_map, map_sem.at[1]),
    ]
    loads = [
        pltpu.make_async_copy(contributions_hbm.at[0, c], contributions.at[c], load_sem.at[c])
        for c in range(comps)
    ]
    fetches = [
        pltpu.make_async_copy(diagonal_hbm.at[pl.ds(mine, half)], diagonal, fetch_sem.at[0]),
        pltpu.make_async_copy(mortar_hbm.at[pl.ds(mine, half)], mortar, fetch_sem.at[1]),
        pltpu.make_async_copy(inverse_hbm.at[pl.ds(mine, half)], inverse, fetch_sem.at[2]),
    ]
    for copy in map_loads + loads + fetches:
        copy.start()

    def stretch(target, first, source, count):
        target[...] = jnp.full(target.shape, -1, jnp.int32)
        for k in range(count):
            ids = source[0:1, (first + k) * cap : (first + k + 1) * cap]
            target[:, k * capp : k * capp + cap] = jnp.broadcast_to(ids, (SUBLANES, cap))

    def row_mask(ids, count):
        shape = (count // SUBLANES, SUBLANES, ids.shape[1])
        rows = lax.broadcasted_iota(jnp.int32, shape, 0) * SUBLANES + lax.broadcasted_iota(
            jnp.int32, shape, 1
        )
        hits = jnp.where(ids[None] == rows, 1.0, 0.0)
        return hits.reshape(count, ids.shape[1]).astype(jnp.bfloat16)

    def column_mask(target, ids):
        lanes = lax.broadcasted_iota(jnp.int32, (LANES, LANES), 1)
        for k in range(target.shape[0] // LANES):
            row = ids[0:1, k * LANES : (k + 1) * LANES]
            column = jnp.broadcast_to(row, (LANES, LANES)).T
            for g in range(target.shape[1] // LANES):
                hits = jnp.where(column == lanes + g * LANES, 1.0, 0.0)
                target[k * LANES : (k + 1) * LANES, g * LANES : (g + 1) * LANES] = hits.astype(
                    jnp.bfloat16
                )

    def wait_bytes(view, sem):
        pltpu.make_async_copy(view, view, sem).wait()

    def remote(source, target, send_sem, recv_sem, device):
        return pltpu.make_async_remote_copy(
            src_ref=source,
            dst_ref=target,
            send_sem=send_sem,
            recv_sem=recv_sem,
            device_id=device,
            device_id_type=MESH,
        )

    live = pl.ds(0, cap)

    def pick(c):
        loads[c].wait()
        going[c] = one_hot_dot(pick_mask[...], contributions[c]).reshape(n, capp, nodes)

    def send_hub(c):
        for j in far_planes:

            def to_hub(k, carry):
                other = lax.rem(line + k, p)
                remote(
                    going.at[c, far_base + j * p + other, live],
                    hub_in.at[c, j, local, live],
                    hub_send.at[c],
                    hub_recv.at[c, j],
                    {"wide": my_hubs + other},
                ).start()
                return carry

            @pl.when(is_outer)
            def _():
                to_hub(0, 0)

            lax.fori_loop(1, p, to_hub, 0)

        @pl.when(is_hub)
        def _():
            for j in range(2):
                hub_in[c, j, local] = going[c, far_base + j * p + line]

    def send_own(c):
        def to_owner(k, carry):
            peer = base + lax.rem(local + k, m)
            remote(
                going.at[c, peer, live],
                coming.at[c, local, live],
                own_send.at[c],
                own_recv.at[c],
                {"wide": peer},
            ).start()
            return carry

        lax.fori_loop(1, m, to_owner, 0)
        coming[c, local] = going[c, me]

    def gather_hub(c):
        @pl.when(is_hub)
        def _():
            for j in far_planes:
                wait_bytes(hub_in.at[c, j, pl.ds(0, m - 1), live], hub_recv.at[c, j])
                dense_out[c, j] = one_hot_dot(
                    hub_sum_mask[j], hub_in[c, j].reshape(slots, nodes)
                )
                for s in range(2):
                    remote(
                        dense_out.at[c, j, pl.ds(s * half, half)],
                        dense_in.at[c, side],
                        dense_send.at[c, j],
                        dense_recv.at[c],
                        {"wide": far_base + j * p + line, "narrow": s},
                    ).start()

    def swap(c):
        return remote(
            sums.at[c, pl.ds(theirs, half)],
            pair.at[c, side],
            pair_send.at[c],
            pair_recv.at[c],
            {"narrow": 1 - side},
        )

    def gather_own(c):
        wait_bytes(coming.at[c, pl.ds(0, m - 1), live], own_recv.at[c])
        sums[c] = one_hot_dot(sum_mask[...], coming[c].reshape(slots, nodes))
        swap(c).start()
        pair[c, side] = sums[c, pl.ds(mine, half), :]

    def swap_back(c):
        return remote(
            fix_pair.at[c, 1 - side],
            fixes.at[c, pl.ds(mine, half)],
            back_send.at[c],
            back_recv.at[c],
            {"narrow": 1 - side},
        )

    def solve(c):
        swap(c).wait()
        wait_bytes(dense_in.at[c], dense_recv.at[c])

        def condense(g, carry):
            first = pl.multiple_of(g * GROUP, GROUP)
            rows = pl.ds(first, GROUP)
            slave = pair[c, 0, rows, :] + dense_in[c, 0, rows, :]
            master = pair[c, 1, rows, :] + dense_in[c, 1, rows, :]
            scale = diagonal[rows, :]
            low = (slave / scale).astype(jnp.bfloat16)
            condensed = master + block_products(low, lambda b: mortar[first + b], False)
            master_fix = block_products(
                condensed.astype(jnp.bfloat16), lambda b: inverse[first + b], True
            )
            slave_fix = (
                block_products(master_fix.astype(jnp.bfloat16), lambda b: mortar[first + b], True)
                / scale
            )
            fix_pair[c, 0, rows, :] = slave_fix
            fix_pair[c, 1, rows, :] = master_fix
            return carry

        lax.fori_loop(0, half // GROUP, condense, 0, unroll=2)
        swap_back(c).start()
        for s in range(2):
            remote(
                fix_pair.at[c, s],
                up_in.at[c, my_plane, pl.ds(mine, half)],
                up_send.at[c],
                up_recv.at[c, my_plane],
                {"wide": far_hub, "narrow": s},
            ).start()
        fixes[c, pl.ds(mine, half), :] = fix_pair[c, side]

    def return_own(c):
        swap_back(c).wait()
        returning[c] = one_hot_dot(spread_mask[...], fixes[c]).reshape(m, capp, nodes)

        def to_source(k, carry):
            peer = lax.rem(local + k, m)
            remote(
                returning.at[c, peer, live],
                returned.at[c, me, live],
                ret_send.at[c],
                ret_recv.at[c],
                {"wide": base + peer},
            ).start()
            return carry

        lax.fori_loop(1, m, to_source, 0)
        returned[c, me] = returning[c, local]

    def return_hub(c):
        @pl.when(is_hub)
        def _():
            for j in far_planes:
                owner = far_base + j * p + line
                wait_bytes(up_in.at[c, j], up_recv.at[c, j])
                relay[c, j] = one_hot_dot(hub_spread_mask[j], up_in[c, j]).reshape(m, capp, nodes)

                def to_source(k, carry):
                    peer = lax.rem(local + k, m)
                    remote(
                        relay.at[c, j, peer, live],
                        returned.at[c, owner, live],
                        relay_send.at[c, j],
                        ret_recv.at[c],
                        {"wide": base + peer},
                    ).start()
                    return carry

                lax.fori_loop(1, m, to_source, 0)
                returned[c, owner] = relay[c, j, local]

    def place(c):
        @pl.when(is_hub)
        def _():
            wait_bytes(returned.at[c, pl.ds(0, n - 3), live], ret_recv.at[c])

        @pl.when(is_outer)
        def _():
            wait_bytes(returned.at[c, pl.ds(0, n - 1), live], ret_recv.at[c])

        out[0, c] = one_hot_dot(place_mask[...], returned[c].reshape(n * capp, nodes))

    map_loads[0].wait()
    stretch(send_row, 0, send_map, n)
    column_mask(pick_mask, send_row)
    map_loads[1].wait()

    @pl.when(upper == 0)
    def _():
        stretch(own_row, 0, arrival_map, m)
        stretch(far_row, m, arrival_map, m)

    @pl.when(upper == 1)
    def _():
        stretch(far_row, 0, arrival_map, m)
        stretch(own_row, m, arrival_map, m)

    pick(0)
    pl.semaphore_wait(barrier, jnp.where(is_hub, m + 6, m + 2))
    send_ids = remote(
        far_row,
        hub_rows.at[my_plane],
        ids_send.at[0],
        ids_recv.at[my_plane],
        {"wide": far_hub},
    )
    send_ids.start()
    send_hub(0)
    send_own(0)
    for c in range(1, comps):
        pick(c)
        send_hub(c)
        send_own(c)

    @pl.when(is_hub)
    def _():
        for j in far_planes:
            wait_bytes(hub_rows.at[j], ids_recv.at[j])
            hub_sum_mask[j] = row_mask(hub_rows[j], blocks)

    gather_hub(0)
    sum_mask[...] = row_mask(own_row[...], blocks)
    column_mask(spread_mask, own_row)
    gather_own(0)
    for fetch in fetches:
        fetch.wait()
    place_mask[...] = row_mask(send_row[...], row_count)
    gather_hub(1)
    solve(0)
    gather_own(1)
    return_own(0)

    @pl.when(is_hub)
    def _():
        for j in range(2):
            column_mask(hub_spread_mask.at[j], hub_rows.at[j])

    gather_hub(2)
    return_hub(0)
    solve(1)
    gather_own(2)
    return_own(1)
    solve(2)
    return_hub(1)
    return_own(2)
    place(0)
    return_hub(2)
    place(1)
    place(2)

    send_ids.wait_send()
    for c in range(comps):
        wait_bytes(going.at[c, pl.ds(0, m - 1), live], own_send.at[c])
        wait_bytes(returning.at[c, pl.ds(0, m - 1), live], ret_send.at[c])
        wait_bytes(fix_pair.at[c], up_send.at[c])

        @pl.when(is_hub)
        def _():
            wait_bytes(going.at[c, pl.ds(0, m - 2), live], hub_send.at[c])
            for j in range(2):
                wait_bytes(dense_out.at[c, j], dense_send.at[c, j])
                wait_bytes(relay.at[c, j, pl.ds(0, m - 1), live], relay_send.at[c, j])

        @pl.when(is_outer)
        def _():
            wait_bytes(going.at[c, pl.ds(0, m), live], hub_send.at[c])


def shards(contributions, send_map, arrival_map, dual_diagonal, mortar, master_inverse):
    n = lax.axis_size("wide")
    _, comps, row_count, nodes = contributions.shape
    blocks = dual_diagonal.shape[0]
    half = blocks // lax.axis_size("narrow")
    m = n // 2
    cap = send_map.shape[1] // n
    capp = -(-cap // SUBLANES) * SUBLANES
    while m * capp % LANES:
        capp += SUBLANES
    slots = m * capp

    f32, bf16, i32 = jnp.float32, jnp.bfloat16, jnp.int32
    dma = pltpu.SemaphoreType.DMA
    return pl.pallas_call(
        functools.partial(kernel, n, cap, capp),
        out_shape=jax.ShapeDtypeStruct((1, comps, row_count, nodes), f32),
        in_specs=[pl.BlockSpec(memory_space=pl.ANY)] * 6,
        out_specs=pl.BlockSpec(memory_space=pltpu.VMEM),
        scratch_shapes=[
            pltpu.VMEM((comps, row_count, nodes), f32),
            pltpu.VMEM((1, n * cap), i32),
            pltpu.VMEM((1, n * cap), i32),
            pltpu.VMEM((half, nodes), f32),
            pltpu.VMEM((half, nodes, nodes), bf16),
            pltpu.VMEM((half, nodes, nodes), bf16),
            pltpu.VMEM((SUBLANES, n * capp), i32),
            pltpu.VMEM((SUBLANES, slots), i32),
            pltpu.VMEM((SUBLANES, slots), i32),
            pltpu.VMEM((2, SUBLANES, slots), i32),
            pltpu.VMEM((n * capp, row_count), bf16),
            pltpu.VMEM((row_count, n * capp), bf16),
            pltpu.VMEM((blocks, slots), bf16),
            pltpu.VMEM((slots, blocks), bf16),
            pltpu.VMEM((2, blocks, slots), bf16),
            pltpu.VMEM((2, slots, blocks), bf16),
            pltpu.VMEM((comps, n, capp, nodes), f32),
            pltpu.VMEM((comps, m, capp, nodes), f32),
            pltpu.VMEM((comps, 2, m, capp, nodes), f32),
            pltpu.VMEM((comps, 2, blocks, nodes), f32),
            pltpu.VMEM((comps, 2, half, nodes), f32),
            pltpu.VMEM((comps, blocks, nodes), f32),
            pltpu.VMEM((comps, 2, half, nodes), f32),
            pltpu.VMEM((comps, 2, half, nodes), f32),
            pltpu.VMEM((comps, blocks, nodes), f32),
            pltpu.VMEM((comps, m, capp, nodes), f32),
            pltpu.VMEM((comps, 2, blocks, nodes), f32),
            pltpu.VMEM((comps, 2, m, capp, nodes), f32),
            pltpu.VMEM((comps, n, capp, nodes), f32),
            dma((comps,)),
            dma((2,)),
            dma((3,)),
            dma((1,)),
            dma((2,)),
            dma((comps,)),
            dma((comps,)),
            dma((comps,)),
            dma((comps, 2)),
            dma((comps, 2)),
            dma((comps,)),
            dma((comps,)),
            dma((comps,)),
            dma((comps,)),
            dma((comps,)),
            dma((comps,)),
            dma((comps, 2)),
            dma((comps,)),
            dma((comps, 2)),
            dma((comps,)),
        ],
        compiler_params=pltpu.CompilerParams(
            collective_id=0, has_side_effects=True, vmem_limit_bytes=48 * 1024 * 1024
        ),
    )(contributions, send_map, arrival_map, dual_diagonal, mortar, master_inverse)


def solution(mesh):
    placed = (
        P("narrow", None, "wide", None),
        P("wide", None),
        P("wide", None),
        P("wide", None),
        P("wide", None, None),
        P("wide", None, None),
    )
    return jax.shard_map(
        shards,
        mesh=mesh,
        in_specs=placed,
        out_specs=P("narrow", None, "wide", None),
        check_vma=False,
    )
```

```python
import functools

import jax
import jax.numpy as jnp
from jax import lax
from jax.experimental import pallas as pl
from jax.experimental.pallas import tpu as pltpu
from jax.sharding import PartitionSpec as P

GROUP = 32
SUBLANES = 8
LANES = 128
PLANES = 4
MESH = pl.DeviceIdType.MESH


def one_hot_dot(mask, values):
    nodes = values.shape[1]
    high = values.astype(jnp.bfloat16)
    low = (values - high.astype(jnp.float32)).astype(jnp.bfloat16)
    both = jnp.dot(mask, jnp.concatenate([high, low], axis=1), preferred_element_type=jnp.float32)
    return both[:, :nodes] + both[:, nodes:]


def block_products(vectors, matrices, transposed):
    nodes = vectors.shape[1]
    rows = lax.broadcasted_iota(jnp.int32, vectors.shape, 0)
    odd = lax.rem(rows, 2) == 1
    total = jnp.zeros(vectors.shape, jnp.float32)
    wide = jnp.concatenate(
        [jnp.where(odd, total, vectors), jnp.where(odd, vectors, total)], axis=1
    ).astype(jnp.bfloat16)
    for b in range(0, vectors.shape[0], 4):
        m0, m1, m2, m3 = (matrices(b + k) for k in range(4))
        if transposed:
            tile = [[m0, m1], [m2, m3]]
        else:
            tile = [[m0, m2], [m1, m3]]
        tile = jnp.concatenate([jnp.concatenate(part, axis=1) for part in tile], axis=0)
        product = lax.dot_general(
            wide,
            tile,
            (((1,), (1 if transposed else 0,)), ((), ())),
            preferred_element_type=jnp.float32,
        )
        first = (rows >= b) & (rows < b + 2)
        second = (rows >= b + 2) & (rows < b + 4)
        total = jnp.where(first, product[:, :nodes], jnp.where(second, product[:, nodes:], total))
    return total


def kernel(
    n,
    cap,
    capp,
    contributions_hbm,
    send_hbm,
    arrival_hbm,
    diagonal_hbm,
    mortar_hbm,
    inverse_hbm,
    out,
    contributions,
    send_map,
    arrival_map,
    diagonal,
    mortar,
    inverse,
    send_row,
    own_row,
    far_row,
    hub_rows,
    pick_mask,
    place_mask,
    sum_mask,
    spread_mask,
    far_spread_mask,
    hub_sum_mask,
    hub_spread_mask,
    going,
    coming,
    hub_in,
    dense_out,
    dense_in,
    sums,
    pair,
    fix_pair,
    fixes,
    returning,
    returning_far,
    up_in,
    relay,
    returned,
    load_sem,
    map_sem,
    fetch_sem,
    ids_send,
    ids_recv,
    own_send,
    own_recv,
    hub_send,
    hub_recv,
    dense_send,
    dense_recv,
    pair_send,
    pair_recv,
    back_send,
    back_recv,
    up_send,
    up_recv,
    ret_send,
    relay_send,
    ret_recv,
):
    me = lax.axis_index("wide")
    side = lax.axis_index("narrow")
    comps, row_count, nodes = out.shape[1:]
    m = n // 2
    p = n // PLANES
    slots = m * capp
    blocks = sums.shape[1]
    half = blocks // 2
    upper = me // m
    local = lax.rem(me, m)
    line = lax.rem(me, p)
    base = upper * m
    far_base = (1 - upper) * m
    my_hubs = (1 + upper) * p
    far_hub = (2 - upper) * p + line
    is_hub = me // p == 1 + upper
    is_outer = jnp.logical_not(is_hub)
    my_plane = local // p
    far_planes = (1 - upper, upper)
    mine = pl.multiple_of(side * half, half)
    theirs = pl.multiple_of((1 - side) * half, half)

    if capp > cap:
        first_pad = cap // SUBLANES * SUBLANES
        pad = pl.ds(first_pad, capp - first_pad)
        empty = jnp.zeros((comps, m, capp - first_pad, nodes), jnp.float32)
        coming[:, :, pad, :] = empty
        hub_in[:, 0, :, pad, :] = empty
        hub_in[:, 1, :, pad, :] = empty
        returned[:, 0:m, pad, :] = empty
        returned[:, m:n, pad, :] = empty

    barrier = pltpu.get_barrier_semaphore()

    def greet(device):
        pl.semaphore_signal(barrier, inc=1, device_id=device, device_id_type=MESH)

    def greet_half(k, carry):
        greet({"wide": base + lax.rem(local + k, m)})
        return carry

    lax.fori_loop(1, m, greet_half, 0)
    greet({"narrow": 1 - side})
    for s in range(2):
        greet({"wide": far_hub, "narrow": s})

    @pl.when(is_hub)
    def _():
        for s in range(2):
            for j in range(2):
                greet({"wide": far_base + j * p + line, "narrow": s})

    map_loads = [
        pltpu.make_async_copy(send_hbm, send_map, map_sem.at[0]),
        pltpu.make_async_copy(arrival_hbm, arrival_map, map_sem.at[1]),
    ]
    loads = [
        pltpu.make_async_copy(contributions_hbm.at[0, c], contributions.at[c], load_sem.at[c])
        for c in range(comps)
    ]
    fetches = [
        pltpu.make_async_copy(diagonal_hbm.at[pl.ds(mine, half)], diagonal, fetch_sem.at[0]),
        pltpu.make_async_copy(mortar_hbm.at[pl.ds(mine, half)], mortar, fetch_sem.at[1]),
        pltpu.make_async_copy(inverse_hbm.at[pl.ds(mine, half)], inverse, fetch_sem.at[2]),
    ]
    for copy in map_loads + loads + fetches:
        copy.start()

    def stretch(target, first, source, count):
        target[...] = jnp.full(target.shape, -1, jnp.int32)
        for k in range(count):
            ids = source[0:1, (first + k) * cap : (first + k + 1) * cap]
            target[:, k * capp : k * capp + cap] = jnp.broadcast_to(ids, (SUBLANES, cap))

    def row_mask(ids, count):
        shape = (count // SUBLANES, SUBLANES, ids.shape[1])
        rows = lax.broadcasted_iota(jnp.int32, shape, 0) * SUBLANES + lax.broadcasted_iota(
            jnp.int32, shape, 1
        )
        hits = jnp.where(ids[None] == rows, 1.0, 0.0)
        return hits.reshape(count, ids.shape[1]).astype(jnp.bfloat16)

    def column_mask(target, ids):
        lanes = lax.broadcasted_iota(jnp.int32, (LANES, LANES), 1)
        for k in range(target.shape[0] // LANES):
            row = ids[0:1, k * LANES : (k + 1) * LANES]
            column = jnp.broadcast_to(row, (LANES, LANES)).T
            for g in range(target.shape[1] // LANES):
                hits = jnp.where(column == lanes + g * LANES, 1.0, 0.0)
                target[k * LANES : (k + 1) * LANES, g * LANES : (g + 1) * LANES] = hits.astype(
                    jnp.bfloat16
                )

    def wait_bytes(view, sem):
        with jax.named_scope("wait"):
            pltpu.make_async_copy(view, view, sem).wait()

    def remote(source, target, send_sem, recv_sem, device):
        return pltpu.make_async_remote_copy(
            src_ref=source,
            dst_ref=target,
            send_sem=send_sem,
            recv_sem=recv_sem,
            device_id=device,
            device_id_type=MESH,
        )

    live = pl.ds(0, cap)
    straight = (comps - 1,)

    def each_peer(send):
        def cross(k, carry):
            send((1 - my_plane) * p + lax.rem(line + k, p))
            return carry

        def along(k, carry):
            send(my_plane * p + lax.rem(line + k, p))
            return carry

        lax.fori_loop(0, p, cross, 0)
        lax.fori_loop(1, p, along, 0)

    def pick(c):
        with jax.named_scope(f"pick{c}"):
            loads[c].wait()
            going[c] = one_hot_dot(pick_mask[...], contributions[c]).reshape(n, capp, nodes)

    def send_hub(c):
        with jax.named_scope(f"send_hub{c}"):
            for j in far_planes:

                def to_hub(k, carry):
                    other = lax.rem(line + k, p)
                    remote(
                        going.at[c, far_base + j * p + other, live],
                        hub_in.at[c, j, local, live],
                        hub_send.at[c],
                        hub_recv.at[c, j],
                        {"wide": my_hubs + other},
                    ).start()
                    return carry

                @pl.when(is_outer)
                def _():
                    to_hub(0, 0)

                lax.fori_loop(1, p, to_hub, 0)

            @pl.when(is_hub)
            def _():
                for j in range(2):
                    hub_in[c, j, local] = going[c, far_base + j * p + line]

    def send_own(c):
        with jax.named_scope(f"send_own{c}"):

            def to_owner(peer):
                remote(
                    going.at[c, base + peer, live],
                    coming.at[c, local, live],
                    own_send.at[c],
                    own_recv.at[c],
                    {"wide": base + peer},
                ).start()

            each_peer(to_owner)
            coming[c, local] = going[c, me]

    def gather_hub(c):
        with jax.named_scope(f"gather_hub{c}"):
            @pl.when(is_hub)
            def _():
                for j in far_planes:
                    wait_bytes(hub_in.at[c, j, pl.ds(0, m - 1), live], hub_recv.at[c, j])
                    dense_out[c, j] = one_hot_dot(
                        hub_sum_mask[j], hub_in[c, j].reshape(slots, nodes)
                    )
                    for s in range(2):
                        remote(
                            dense_out.at[c, j, pl.ds(s * half, half)],
                            dense_in.at[c, side],
                            dense_send.at[c, j],
                            dense_recv.at[c],
                            {"wide": far_base + j * p + line, "narrow": s},
                        ).start()

    def swap(c):
        return remote(
            sums.at[c, pl.ds(theirs, half)],
            pair.at[c, side],
            pair_send.at[c],
            pair_recv.at[c],
            {"narrow": 1 - side},
        )

    def gather_own(c):
        with jax.named_scope(f"gather_own{c}"):
            wait_bytes(coming.at[c, pl.ds(0, m - 1), live], own_recv.at[c])
            sums[c] = one_hot_dot(sum_mask[...], coming[c].reshape(slots, nodes))
            swap(c).start()
            pair[c, side] = sums[c, pl.ds(mine, half), :]

    def swap_back(c):
        return remote(
            fix_pair.at[c, 1 - side],
            fixes.at[c, pl.ds(mine, half)],
            back_send.at[c],
            back_recv.at[c],
            {"narrow": 1 - side},
        )

    def solve(c):
        with jax.named_scope(f"solve{c}"):
            with jax.named_scope("wait_swap"):
                swap(c).wait()
            wait_bytes(dense_in.at[c], dense_recv.at[c])

            def condense(g, carry):
                first = pl.multiple_of(g * GROUP, GROUP)
                rows = pl.ds(first, GROUP)
                slave = pair[c, 0, rows, :] + dense_in[c, 0, rows, :]
                master = pair[c, 1, rows, :] + dense_in[c, 1, rows, :]
                scale = diagonal[rows, :]
                condensed = master + block_products(slave / scale, lambda b: mortar[first + b], False)
                master_fix = block_products(condensed, lambda b: inverse[first + b], True)
                slave_fix = block_products(master_fix, lambda b: mortar[first + b], True) / scale
                fix_pair[c, 0, rows, :] = slave_fix
                fix_pair[c, 1, rows, :] = master_fix
                return carry

            lax.fori_loop(0, half // GROUP, condense, 0, unroll=2)
            swap_back(c).start()
            if c not in straight:
                for s in range(2):
                    remote(
                        fix_pair.at[c, s],
                        up_in.at[c, my_plane, pl.ds(mine, half)],
                        up_send.at[c],
                        up_recv.at[c, my_plane],
                        {"wide": far_hub, "narrow": s},
                    ).start()
            fixes[c, pl.ds(mine, half), :] = fix_pair[c, side]

    def return_own(c):
        with jax.named_scope(f"return_own{c}"):
            with jax.named_scope("wait_back"):
                swap_back(c).wait()
            if c in straight:
                returning_far[c] = one_hot_dot(far_spread_mask[...], fixes[c]).reshape(
                    m, capp, nodes
                )

                def to_far(k, carry):
                    peer = lax.rem(local + k, m)
                    remote(
                        returning_far.at[c, peer, live],
                        returned.at[c, me, live],
                        ret_send.at[c],
                        ret_recv.at[c],
                        {"wide": far_base + peer},
                    ).start()
                    return carry

                lax.fori_loop(0, m, to_far, 0)
            returning[c] = one_hot_dot(spread_mask[...], fixes[c]).reshape(m, capp, nodes)

            def to_source(peer):
                remote(
                    returning.at[c, peer, live],
                    returned.at[c, me, live],
                    ret_send.at[c],
                    ret_recv.at[c],
                    {"wide": base + peer},
                ).start()

            each_peer(to_source)
            returned[c, me] = returning[c, local]

    def return_hub(c):
        @pl.when(is_hub)
        def _():
            with jax.named_scope(f"return_hub{c}"):
                for j in far_planes:
                    owner = far_base + j * p + line
                    wait_bytes(up_in.at[c, j], up_recv.at[c, j])
                    relay[c, j] = one_hot_dot(hub_spread_mask[j], up_in[c, j]).reshape(
                        m, capp, nodes
                    )

                    def to_source(peer):
                        remote(
                            relay.at[c, j, peer, live],
                            returned.at[c, owner, live],
                            relay_send.at[c, j],
                            ret_recv.at[c],
                            {"wide": base + peer},
                        ).start()

                    each_peer(to_source)
                    returned[c, owner] = relay[c, j, local]

    def place(c):
        with jax.named_scope(f"place{c}"):
            if c in straight:
                wait_bytes(returned.at[c, pl.ds(0, n - 1), live], ret_recv.at[c])
            else:

                @pl.when(is_hub)
                def _():
                    wait_bytes(returned.at[c, pl.ds(0, n - 3), live], ret_recv.at[c])

                @pl.when(is_outer)
                def _():
                    wait_bytes(returned.at[c, pl.ds(0, n - 1), live], ret_recv.at[c])

            out[0, c] = one_hot_dot(place_mask[...], returned[c].reshape(n * capp, nodes))

    map_loads[0].wait()
    with jax.named_scope("pick_mask"):
        stretch(send_row, 0, send_map, n)
        column_mask(pick_mask, send_row)
    map_loads[1].wait()

    @pl.when(upper == 0)
    def _():
        stretch(own_row, 0, arrival_map, m)
        stretch(far_row, m, arrival_map, m)

    @pl.when(upper == 1)
    def _():
        stretch(far_row, 0, arrival_map, m)
        stretch(own_row, m, arrival_map, m)

    pick(0)
    with jax.named_scope("entry"):
        pl.semaphore_wait(barrier, jnp.where(is_hub, m + 6, m + 2))
    send_ids = remote(
        far_row,
        hub_rows.at[my_plane],
        ids_send.at[0],
        ids_recv.at[my_plane],
        {"wide": far_hub},
    )
    send_ids.start()
    send_hub(0)
    for c in range(1, comps):
        pick(c)
        send_hub(c)
        send_own(c - 1)
    send_own(comps - 1)

    @pl.when(is_hub)
    def _():
        with jax.named_scope("hub_sum_mask"):
            for j in far_planes:
                wait_bytes(hub_rows.at[j], ids_recv.at[j])
                hub_sum_mask[j] = row_mask(hub_rows[j], blocks)

    gather_hub(0)
    with jax.named_scope("own_masks"):
        sum_mask[...] = row_mask(own_row[...], blocks)
        column_mask(spread_mask, own_row)
        column_mask(far_spread_mask, far_row)
    gather_own(0)
    for fetch in fetches:
        fetch.wait()
    with jax.named_scope("place_mask"):
        place_mask[...] = row_mask(send_row[...], row_count)
    gather_hub(1)
    solve(0)
    gather_own(1)
    return_own(0)

    @pl.when(is_hub)
    def _():
        with jax.named_scope("hub_spread_mask"):
            for j in range(2):
                column_mask(hub_spread_mask.at[j], hub_rows.at[j])

    gather_hub(2)
    solve(1)
    gather_own(2)
    return_hub(0)
    return_own(1)
    return_hub(1)
    solve(2)
    return_own(2)
    place(0)
    place(1)
    place(2)

    with jax.named_scope("drain"):
        send_ids.wait_send()
        for c in range(comps):
            wait_bytes(going.at[c, pl.ds(0, m - 1), live], own_send.at[c])
            if c in straight:
                wait_bytes(going.at[c, pl.ds(0, n - 1), live], ret_send.at[c])
            else:
                wait_bytes(returning.at[c, pl.ds(0, m - 1), live], ret_send.at[c])
                wait_bytes(fix_pair.at[c], up_send.at[c])

            @pl.when(is_hub)
            def _():
                wait_bytes(going.at[c, pl.ds(0, m - 2), live], hub_send.at[c])
                for j in range(2):
                    wait_bytes(dense_out.at[c, j], dense_send.at[c, j])
                    if c not in straight:
                        wait_bytes(relay.at[c, j, pl.ds(0, m - 1), live], relay_send.at[c, j])

            @pl.when(is_outer)
            def _():
                wait_bytes(going.at[c, pl.ds(0, m), live], hub_send.at[c])


def shards(contributions, send_map, arrival_map, dual_diagonal, mortar, master_inverse):
    n = lax.axis_size("wide")
    _, comps, row_count, nodes = contributions.shape
    blocks = dual_diagonal.shape[0]
    half = blocks // lax.axis_size("narrow")
    m = n // 2
    cap = send_map.shape[1] // n
    capp = -(-cap // SUBLANES) * SUBLANES
    while m * capp % LANES:
        capp += SUBLANES
    slots = m * capp

    f32, bf16, i32 = jnp.float32, jnp.bfloat16, jnp.int32
    dma = pltpu.SemaphoreType.DMA
    return pl.pallas_call(
        functools.partial(kernel, n, cap, capp),
        out_shape=jax.ShapeDtypeStruct((1, comps, row_count, nodes), f32),
        in_specs=[pl.BlockSpec(memory_space=pltpu.HBM)] * 6,
        out_specs=pl.BlockSpec(memory_space=pltpu.VMEM),
        scratch_shapes=[
            pltpu.VMEM((comps, row_count, nodes), f32),
            pltpu.VMEM((1, n * cap), i32),
            pltpu.VMEM((1, n * cap), i32),
            pltpu.VMEM((half, nodes), f32),
            pltpu.VMEM((half, nodes, nodes), bf16),
            pltpu.VMEM((half, nodes, nodes), bf16),
            pltpu.VMEM((SUBLANES, n * capp), i32),
            pltpu.VMEM((SUBLANES, slots), i32),
            pltpu.VMEM((SUBLANES, slots), i32),
            pltpu.VMEM((2, SUBLANES, slots), i32),
            pltpu.VMEM((n * capp, row_count), bf16),
            pltpu.VMEM((row_count, n * capp), bf16),
            pltpu.VMEM((blocks, slots), bf16),
            pltpu.VMEM((slots, blocks), bf16),
            pltpu.VMEM((slots, blocks), bf16),
            pltpu.VMEM((2, blocks, slots), bf16),
            pltpu.VMEM((2, slots, blocks), bf16),
            pltpu.VMEM((comps, n, capp, nodes), f32),
            pltpu.VMEM((comps, m, capp, nodes), f32),
            pltpu.VMEM((comps, 2, m, capp, nodes), f32),
            pltpu.VMEM((comps, 2, blocks, nodes), f32),
            pltpu.VMEM((comps, 2, half, nodes), f32),
            pltpu.VMEM((comps, blocks, nodes), f32),
            pltpu.VMEM((comps, 2, half, nodes), f32),
            pltpu.VMEM((comps, 2, half, nodes), f32),
            pltpu.VMEM((comps, blocks, nodes), f32),
            pltpu.VMEM((comps, m, capp, nodes), f32),
            pltpu.VMEM((comps, m, capp, nodes), f32),
            pltpu.VMEM((comps, 2, blocks, nodes), f32),
            pltpu.VMEM((comps, 2, m, capp, nodes), f32),
            pltpu.VMEM((comps, n, capp, nodes), f32),
            dma((comps,)),
            dma((2,)),
            dma((3,)),
            dma((1,)),
            dma((2,)),
            dma((comps,)),
            dma((comps,)),
            dma((comps,)),
            dma((comps, 2)),
            dma((comps, 2)),
            dma((comps,)),
            dma((comps,)),
            dma((comps,)),
            dma((comps,)),
            dma((comps,)),
            dma((comps,)),
            dma((comps, 2)),
            dma((comps,)),
            dma((comps, 2)),
            dma((comps,)),
        ],
        compiler_params=pltpu.CompilerParams(
            collective_id=0, has_side_effects=True, vmem_limit_bytes=67043328
        ),
    )(contributions, send_map, arrival_map, dual_diagonal, mortar, master_inverse)


def solution(mesh):
    placed = (
        P("narrow", None, "wide", None),
        P("wide", None),
        P("wide", None),
        P("wide", None),
        P("wide", None, None),
        P("wide", None, None),
    )
    return jax.shard_map(
        shards,
        mesh=mesh,
        in_specs=placed,
        out_specs=P("narrow", None, "wide", None),
        check_vma=False,
    )
```

```python
import functools

import jax
import jax.numpy as jnp
from jax import lax
from jax.experimental import pallas as pl
from jax.experimental.pallas import tpu as pltpu
from jax.sharding import PartitionSpec as P

GROUP = 32
SUBLANES = 8
LANES = 128
PLANES = 4
MESH = pl.DeviceIdType.MESH


def one_hot_dot(mask, values):
    nodes = values.shape[1]
    high = values.astype(jnp.bfloat16)
    low = (values - high.astype(jnp.float32)).astype(jnp.bfloat16)
    both = jnp.dot(mask, jnp.concatenate([high, low], axis=1), preferred_element_type=jnp.float32)
    return both[:, :nodes] + both[:, nodes:]


def block_products(vectors, matrices, transposed):
    nodes = vectors.shape[1]
    rows = lax.broadcasted_iota(jnp.int32, vectors.shape, 0)
    odd = lax.rem(rows, 2) == 1
    total = jnp.zeros(vectors.shape, jnp.float32)
    wide = jnp.concatenate(
        [jnp.where(odd, total, vectors), jnp.where(odd, vectors, total)], axis=1
    ).astype(jnp.bfloat16)
    for b in range(0, vectors.shape[0], 4):
        m0, m1, m2, m3 = (matrices(b + k) for k in range(4))
        if transposed:
            tile = [[m0, m1], [m2, m3]]
        else:
            tile = [[m0, m2], [m1, m3]]
        tile = jnp.concatenate([jnp.concatenate(part, axis=1) for part in tile], axis=0)
        product = lax.dot_general(
            wide,
            tile,
            (((1,), (1 if transposed else 0,)), ((), ())),
            preferred_element_type=jnp.float32,
        )
        first = (rows >= b) & (rows < b + 2)
        second = (rows >= b + 2) & (rows < b + 4)
        total = jnp.where(first, product[:, :nodes], jnp.where(second, product[:, nodes:], total))
    return total


def kernel(
    n,
    cap,
    capp,
    contributions_hbm,
    send_hbm,
    arrival_hbm,
    diagonal_hbm,
    mortar_hbm,
    inverse_hbm,
    out,
    contributions,
    send_map,
    arrival_map,
    diagonal,
    mortar,
    inverse,
    send_row,
    own_row,
    far_row,
    hub_rows,
    pick_mask,
    place_mask,
    sum_mask,
    spread_mask,
    far_spread_mask,
    hub_sum_mask,
    hub_spread_mask,
    going,
    coming,
    hub_in,
    dense_out,
    dense_in,
    sums,
    pair,
    fix_pair,
    fixes,
    returning,
    returning_far,
    up_in,
    relay,
    returned,
    load_sem,
    map_sem,
    fetch_sem,
    ids_send,
    ids_recv,
    own_send,
    own_recv,
    hub_send,
    hub_recv,
    dense_send,
    dense_recv,
    pair_send,
    pair_recv,
    back_send,
    back_recv,
    up_send,
    up_recv,
    ret_send,
    relay_send,
    ret_recv,
):
    me = lax.axis_index("wide")
    side = lax.axis_index("narrow")
    comps, row_count, nodes = out.shape[1:]
    m = n // 2
    p = n // PLANES
    slots = m * capp
    blocks = sums.shape[1]
    half = blocks // 2
    upper = me // m
    local = lax.rem(me, m)
    line = lax.rem(me, p)
    base = upper * m
    far_base = (1 - upper) * m
    my_hubs = (1 + upper) * p
    far_hub = (2 - upper) * p + line
    is_hub = me // p == 1 + upper
    is_outer = jnp.logical_not(is_hub)
    my_plane = local // p
    far_planes = (1 - upper, upper)
    mine = pl.multiple_of(side * half, half)
    theirs = pl.multiple_of((1 - side) * half, half)

    if capp > cap:
        first_pad = cap // SUBLANES * SUBLANES
        pad = pl.ds(first_pad, capp - first_pad)
        empty = jnp.zeros((comps, m, capp - first_pad, nodes), jnp.float32)
        coming[:, :, pad, :] = empty
        hub_in[:, 0, :, pad, :] = empty
        hub_in[:, 1, :, pad, :] = empty
        returned[:, 0:m, pad, :] = empty
        returned[:, m:n, pad, :] = empty

    barrier = pltpu.get_barrier_semaphore()

    def greet(device):
        pl.semaphore_signal(barrier, inc=1, device_id=device, device_id_type=MESH)

    def greet_half(k, carry):
        greet({"wide": base + lax.rem(local + k, m)})
        return carry

    lax.fori_loop(1, m, greet_half, 0)
    greet({"narrow": 1 - side})
    for s in range(2):
        greet({"wide": far_hub, "narrow": s})

    @pl.when(is_hub)
    def _():
        for s in range(2):
            for j in range(2):
                greet({"wide": far_base + j * p + line, "narrow": s})

    map_loads = [
        pltpu.make_async_copy(send_hbm, send_map, map_sem.at[0]),
        pltpu.make_async_copy(arrival_hbm, arrival_map, map_sem.at[1]),
    ]
    loads = [
        pltpu.make_async_copy(contributions_hbm.at[0, c], contributions.at[c], load_sem.at[c])
        for c in range(comps)
    ]
    fetches = [
        pltpu.make_async_copy(diagonal_hbm.at[pl.ds(mine, half)], diagonal, fetch_sem.at[0]),
        pltpu.make_async_copy(mortar_hbm.at[pl.ds(mine, half)], mortar, fetch_sem.at[1]),
        pltpu.make_async_copy(inverse_hbm.at[pl.ds(mine, half)], inverse, fetch_sem.at[2]),
    ]
    for copy in map_loads + loads:
        copy.start()

    def stretch(target, first, source, count):
        target[...] = jnp.full(target.shape, -1, jnp.int32)
        for k in range(count):
            ids = source[0:1, (first + k) * cap : (first + k + 1) * cap]
            target[:, k * capp : k * capp + cap] = jnp.broadcast_to(ids, (SUBLANES, cap))

    def row_mask(ids, count):
        shape = (count // SUBLANES, SUBLANES, ids.shape[1])
        rows = lax.broadcasted_iota(jnp.int32, shape, 0) * SUBLANES + lax.broadcasted_iota(
            jnp.int32, shape, 1
        )
        hits = jnp.where(ids[None] == rows, 1.0, 0.0)
        return hits.reshape(count, ids.shape[1]).astype(jnp.bfloat16)

    def column_mask(target, ids):
        lanes = lax.broadcasted_iota(jnp.int32, (LANES, LANES), 1)
        for k in range(target.shape[0] // LANES):
            row = ids[0:1, k * LANES : (k + 1) * LANES]
            column = jnp.broadcast_to(row, (LANES, LANES)).T
            for g in range(target.shape[1] // LANES):
                hits = jnp.where(column == lanes + g * LANES, 1.0, 0.0)
                target[k * LANES : (k + 1) * LANES, g * LANES : (g + 1) * LANES] = hits.astype(
                    jnp.bfloat16
                )

    def wait_bytes(view, sem):
        with jax.named_scope("wait"):
            pltpu.make_async_copy(view, view, sem).wait()

    def remote(source, target, send_sem, recv_sem, device):
        return pltpu.make_async_remote_copy(
            src_ref=source,
            dst_ref=target,
            send_sem=send_sem,
            recv_sem=recv_sem,
            device_id=device,
            device_id_type=MESH,
        )

    live = pl.ds(0, cap)
    straight_back = tuple(range(1, comps))

    def back_planes(c):
        return far_planes[:1] if c in straight_back else far_planes

    def each_peer(send):
        def cross(k, carry):
            send((1 - my_plane) * p + lax.rem(line + k, p))
            return carry

        def along(k, carry):
            send(my_plane * p + lax.rem(line + k, p))
            return carry

        lax.fori_loop(0, p, cross, 0)
        lax.fori_loop(1, p, along, 0)

    def pick(c):
        with jax.named_scope(f"pick{c}"):
            loads[c].wait()
            going[c] = one_hot_dot(pick_mask[...], contributions[c]).reshape(n, capp, nodes)

    def send_hub(c):
        with jax.named_scope(f"send_hub{c}"):
            for j in far_planes:

                def to_hub(k, carry):
                    other = lax.rem(line + k, p)
                    remote(
                        going.at[c, far_base + j * p + other, live],
                        hub_in.at[c, j, local, live],
                        hub_send.at[c],
                        hub_recv.at[c, j],
                        {"wide": my_hubs + other},
                    ).start()
                    return carry

                @pl.when(is_outer)
                def _():
                    to_hub(0, 0)

                lax.fori_loop(1, p, to_hub, 0)

            @pl.when(is_hub)
            def _():
                for j in range(2):
                    hub_in[c, j, local] = going[c, far_base + j * p + line]

    def send_own(c):
        with jax.named_scope(f"send_own{c}"):

            def to_owner(peer):
                remote(
                    going.at[c, base + peer, live],
                    coming.at[c, local, live],
                    own_send.at[c],
                    own_recv.at[c],
                    {"wide": base + peer},
                ).start()

            each_peer(to_owner)
            coming[c, local] = going[c, me]

    def gather_hub(c):
        with jax.named_scope(f"gather_hub{c}"):
            @pl.when(is_hub)
            def _():
                for j in far_planes:
                    wait_bytes(hub_in.at[c, j, pl.ds(0, m - 1), live], hub_recv.at[c, j])
                    dense_out[c, j] = one_hot_dot(
                        hub_sum_mask[j], hub_in[c, j].reshape(slots, nodes)
                    )
                    for s in range(2):
                        remote(
                            dense_out.at[c, j, pl.ds(s * half, half)],
                            dense_in.at[c, side],
                            dense_send.at[c, j],
                            dense_recv.at[c],
                            {"wide": far_base + j * p + line, "narrow": s},
                        ).start()

    def swap(c):
        return remote(
            sums.at[c, pl.ds(theirs, half)],
            pair.at[c, side],
            pair_send.at[c],
            pair_recv.at[c],
            {"narrow": 1 - side},
        )

    def gather_own(c):
        with jax.named_scope(f"gather_own{c}"):
            wait_bytes(coming.at[c, pl.ds(0, m - 1), live], own_recv.at[c])
            sums[c] = one_hot_dot(sum_mask[...], coming[c].reshape(slots, nodes))
            swap(c).start()
            pair[c, side] = sums[c, pl.ds(mine, half), :]

    def swap_back(c):
        return remote(
            fix_pair.at[c, 1 - side],
            fixes.at[c, pl.ds(mine, half)],
            back_send.at[c],
            back_recv.at[c],
            {"narrow": 1 - side},
        )

    def solve(c):
        with jax.named_scope(f"solve{c}"):
            with jax.named_scope("wait_swap"):
                swap(c).wait()
            wait_bytes(dense_in.at[c], dense_recv.at[c])

            def condense(g, carry):
                first = pl.multiple_of(g * GROUP, GROUP)
                rows = pl.ds(first, GROUP)
                slave = pair[c, 0, rows, :] + dense_in[c, 0, rows, :]
                master = pair[c, 1, rows, :] + dense_in[c, 1, rows, :]
                scale = diagonal[rows, :]
                condensed = master + block_products(slave / scale, lambda b: mortar[first + b], False)
                master_fix = block_products(condensed, lambda b: inverse[first + b], True)
                slave_fix = block_products(master_fix, lambda b: mortar[first + b], True) / scale
                fix_pair[c, 0, rows, :] = slave_fix
                fix_pair[c, 1, rows, :] = master_fix
                return carry

            lax.fori_loop(0, half // GROUP, condense, 0, unroll=2)
            swap_back(c).start()

            def to_far_hub():
                for s in range(2):
                    remote(
                        fix_pair.at[c, s],
                        up_in.at[c, my_plane, pl.ds(mine, half)],
                        up_send.at[c],
                        up_recv.at[c, my_plane],
                        {"wide": far_hub, "narrow": s},
                    ).start()

            if c in straight_back:
                pl.when(is_outer)(to_far_hub)
            else:
                to_far_hub()
            fixes[c, pl.ds(mine, half), :] = fix_pair[c, side]

    def return_own(c):
        with jax.named_scope(f"return_own{c}"):
            with jax.named_scope("wait_back"):
                swap_back(c).wait()
            if c in straight_back:

                @pl.when(is_hub)
                def _():
                    returning_far[c] = one_hot_dot(far_spread_mask[...], fixes[c]).reshape(
                        m, capp, nodes
                    )

                    def to_far(k, carry):
                        peer = lax.rem(local + k, m)
                        remote(
                            returning_far.at[c, peer, live],
                            returned.at[c, me, live],
                            ret_send.at[c],
                            ret_recv.at[c],
                            {"wide": far_base + peer},
                        ).start()
                        return carry

                    lax.fori_loop(0, m, to_far, 0)

            returning[c] = one_hot_dot(spread_mask[...], fixes[c]).reshape(m, capp, nodes)

            def to_source(peer):
                remote(
                    returning.at[c, peer, live],
                    returned.at[c, me, live],
                    ret_send.at[c],
                    ret_recv.at[c],
                    {"wide": base + peer},
                ).start()

            each_peer(to_source)
            returned[c, me] = returning[c, local]

    def return_hub(c):
        @pl.when(is_hub)
        def _():
            with jax.named_scope(f"return_hub{c}"):
                for j in back_planes(c):
                    owner = far_base + j * p + line
                    wait_bytes(up_in.at[c, j], up_recv.at[c, j])
                    relay[c, j] = one_hot_dot(hub_spread_mask[j], up_in[c, j]).reshape(
                        m, capp, nodes
                    )

                    def to_source(peer):
                        remote(
                            relay.at[c, j, peer, live],
                            returned.at[c, owner, live],
                            relay_send.at[c, j],
                            ret_recv.at[c],
                            {"wide": base + peer},
                        ).start()

                    each_peer(to_source)
                    returned[c, owner] = relay[c, j, local]

    def place(c):
        with jax.named_scope(f"place{c}"):
            at_hub = len(back_planes(c))

            @pl.when(is_hub)
            def _():
                wait_bytes(returned.at[c, pl.ds(0, n - 1 - at_hub), live], ret_recv.at[c])

            @pl.when(is_outer)
            def _():
                wait_bytes(returned.at[c, pl.ds(0, n - 1), live], ret_recv.at[c])

            out[0, c] = one_hot_dot(place_mask[...], returned[c].reshape(n * capp, nodes))

    map_loads[0].wait()
    with jax.named_scope("pick_mask"):
        stretch(send_row, 0, send_map, n)
        column_mask(pick_mask, send_row)
    map_loads[1].wait()

    pick(0)
    for fetch in fetches:
        fetch.start()
    with jax.named_scope("rows"):

        @pl.when(upper == 0)
        def _():
            stretch(own_row, 0, arrival_map, m)
            stretch(far_row, m, arrival_map, m)

        @pl.when(upper == 1)
        def _():
            stretch(far_row, 0, arrival_map, m)
            stretch(own_row, m, arrival_map, m)

    with jax.named_scope("entry"):
        pl.semaphore_wait(barrier, jnp.where(is_hub, m + 6, m + 2))
    send_ids = remote(
        far_row,
        hub_rows.at[my_plane],
        ids_send.at[0],
        ids_recv.at[my_plane],
        {"wide": far_hub},
    )
    send_ids.start()
    send_hub(0)
    pick(1)
    send_hub(1)
    send_own(0)
    pick(2)
    send_hub(2)
    send_own(1)
    send_own(2)
    with jax.named_scope("own_masks"):
        sum_mask[...] = row_mask(own_row[...], blocks)
        column_mask(spread_mask, own_row)

    @pl.when(is_hub)
    def _():
        with jax.named_scope("hub_masks"):
            column_mask(far_spread_mask, far_row)
            for j in far_planes:
                wait_bytes(hub_rows.at[j], ids_recv.at[j])
                hub_sum_mask[j] = row_mask(hub_rows[j], blocks)
                column_mask(hub_spread_mask.at[j], hub_rows.at[j])

    gather_hub(0)
    with jax.named_scope("place_mask"):
        place_mask[...] = row_mask(send_row[...], row_count)
    gather_hub(1)
    gather_own(0)
    for fetch in fetches:
        fetch.wait()
    solve(0)
    gather_hub(2)
    gather_own(1)
    return_own(0)
    solve(1)
    gather_own(2)
    return_hub(0)
    return_own(1)
    return_hub(1)
    solve(2)
    return_own(2)
    return_hub(2)
    place(0)
    place(1)
    place(2)

    with jax.named_scope("drain"):
        send_ids.wait_send()
        for c in range(comps):
            wait_bytes(going.at[c, pl.ds(0, m - 1), live], own_send.at[c])

            @pl.when(is_hub)
            def _():
                wait_bytes(going.at[c, pl.ds(0, m - 2), live], hub_send.at[c])
                for j in range(2):
                    wait_bytes(dense_out.at[c, j], dense_send.at[c, j])
                for j in back_planes(c):
                    wait_bytes(relay.at[c, j, pl.ds(0, m - 1), live], relay_send.at[c, j])
                if c in straight_back:
                    wait_bytes(going.at[c, pl.ds(0, n - 1), live], ret_send.at[c])
                else:
                    wait_bytes(going.at[c, pl.ds(0, m - 1), live], ret_send.at[c])
                    wait_bytes(fix_pair.at[c], up_send.at[c])

            @pl.when(is_outer)
            def _():
                wait_bytes(going.at[c, pl.ds(0, m), live], hub_send.at[c])
                wait_bytes(going.at[c, pl.ds(0, m - 1), live], ret_send.at[c])
                wait_bytes(fix_pair.at[c], up_send.at[c])


def shards(contributions, send_map, arrival_map, dual_diagonal, mortar, master_inverse):
    n = lax.axis_size("wide")
    _, comps, row_count, nodes = contributions.shape
    blocks = dual_diagonal.shape[0]
    half = blocks // lax.axis_size("narrow")
    m = n // 2
    cap = send_map.shape[1] // n
    capp = -(-cap // SUBLANES) * SUBLANES
    while m * capp % LANES:
        capp += SUBLANES
    slots = m * capp

    operands = tuple(
        pltpu.with_memory_space_constraint(x, pltpu.HBM)
        for x in (contributions, send_map, arrival_map, dual_diagonal, mortar, master_inverse)
    )
    f32, bf16, i32 = jnp.float32, jnp.bfloat16, jnp.int32
    dma = pltpu.SemaphoreType.DMA
    return pl.pallas_call(
        functools.partial(kernel, n, cap, capp),
        out_shape=jax.ShapeDtypeStruct((1, comps, row_count, nodes), f32),
        in_specs=[pl.BlockSpec(memory_space=pltpu.HBM)] * 6,
        out_specs=pl.BlockSpec(memory_space=pltpu.VMEM),
        scratch_shapes=[
            pltpu.VMEM((comps, row_count, nodes), f32),
            pltpu.VMEM((1, n * cap), i32),
            pltpu.VMEM((1, n * cap), i32),
            pltpu.VMEM((half, nodes), f32),
            pltpu.VMEM((half, nodes, nodes), bf16),
            pltpu.VMEM((half, nodes, nodes), bf16),
            pltpu.VMEM((SUBLANES, n * capp), i32),
            pltpu.VMEM((SUBLANES, slots), i32),
            pltpu.VMEM((SUBLANES, slots), i32),
            pltpu.VMEM((2, SUBLANES, slots), i32),
            pltpu.VMEM((n * capp, row_count), bf16),
            pltpu.VMEM((row_count, n * capp), bf16),
            pltpu.VMEM((blocks, slots), bf16),
            pltpu.VMEM((slots, blocks), bf16),
            pltpu.VMEM((slots, blocks), bf16),
            pltpu.VMEM((2, blocks, slots), bf16),
            pltpu.VMEM((2, slots, blocks), bf16),
            pltpu.VMEM((comps, n, capp, nodes), f32),
            pltpu.VMEM((comps, m, capp, nodes), f32),
            pltpu.VMEM((comps, 2, m, capp, nodes), f32),
            pltpu.VMEM((comps, 2, blocks, nodes), f32),
            pltpu.VMEM((comps, 2, half, nodes), f32),
            pltpu.VMEM((comps, blocks, nodes), f32),
            pltpu.VMEM((comps, 2, half, nodes), f32),
            pltpu.VMEM((comps, 2, half, nodes), f32),
            pltpu.VMEM((comps, blocks, nodes), f32),
            pltpu.VMEM((comps, m, capp, nodes), f32),
            pltpu.VMEM((comps, m, capp, nodes), f32),
            pltpu.VMEM((comps, 2, blocks, nodes), f32),
            pltpu.VMEM((comps, 2, m, capp, nodes), f32),
            pltpu.VMEM((comps, n, capp, nodes), f32),
            dma((comps,)),
            dma((2,)),
            dma((3,)),
            dma((1,)),
            dma((2,)),
            dma((comps,)),
            dma((comps,)),
            dma((comps,)),
            dma((comps, 2)),
            dma((comps, 2)),
            dma((comps,)),
            dma((comps,)),
            dma((comps,)),
            dma((comps,)),
            dma((comps,)),
            dma((comps,)),
            dma((comps, 2)),
            dma((comps,)),
            dma((comps, 2)),
            dma((comps,)),
        ],
        compiler_params=pltpu.CompilerParams(
            collective_id=0, has_side_effects=True, vmem_limit_bytes=48 * 1024 * 1024
        ),
    )(*operands)


def solution(mesh):
    placed = (
        P("narrow", None, "wide", None),
        P("wide", None),
        P("wide", None),
        P("wide", None),
        P("wide", None, None),
        P("wide", None, None),
    )
    return jax.shard_map(
        shards,
        mesh=mesh,
        in_specs=placed,
        out_specs=P("narrow", None, "wide", None),
        check_vma=False,
    )
```

```python
import functools

import jax
import jax.numpy as jnp
from jax import lax
from jax.experimental import pallas as pl
from jax.experimental.pallas import tpu as pltpu
from jax.sharding import PartitionSpec as P

GROUP = 32
SUBLANES = 8
LANES = 128
PLANES = 4
MESH = pl.DeviceIdType.MESH


def one_hot_dot(mask, values):
    nodes = values.shape[1]
    high = values.astype(jnp.bfloat16)
    low = (values - high.astype(jnp.float32)).astype(jnp.bfloat16)
    both = jnp.dot(mask, jnp.concatenate([high, low], axis=1), preferred_element_type=jnp.float32)
    return both[:, :nodes] + both[:, nodes:]


def block_products(vectors, matrices, transposed):
    nodes = vectors.shape[1]
    rows = lax.broadcasted_iota(jnp.int32, vectors.shape, 0)
    odd = lax.rem(rows, 2) == 1
    total = jnp.zeros(vectors.shape, jnp.float32)
    wide = jnp.concatenate(
        [jnp.where(odd, total, vectors), jnp.where(odd, vectors, total)], axis=1
    ).astype(jnp.bfloat16)
    for b in range(0, vectors.shape[0], 4):
        m0, m1, m2, m3 = (matrices(b + k) for k in range(4))
        if transposed:
            tile = [[m0, m1], [m2, m3]]
        else:
            tile = [[m0, m2], [m1, m3]]
        tile = jnp.concatenate([jnp.concatenate(part, axis=1) for part in tile], axis=0)
        product = lax.dot_general(
            wide,
            tile,
            (((1,), (1 if transposed else 0,)), ((), ())),
            preferred_element_type=jnp.float32,
        )
        first = (rows >= b) & (rows < b + 2)
        second = (rows >= b + 2) & (rows < b + 4)
        total = jnp.where(first, product[:, :nodes], jnp.where(second, product[:, nodes:], total))
    return total


def kernel(
    n,
    cap,
    capp,
    contributions_hbm,
    send_hbm,
    arrival_hbm,
    diagonal_hbm,
    mortar_hbm,
    inverse_hbm,
    out,
    contributions,
    send_map,
    arrival_map,
    diagonal,
    mortar,
    inverse,
    send_row,
    own_row,
    far_row,
    hub_rows,
    pick_mask,
    place_mask,
    sum_mask,
    spread_mask,
    far_spread_mask,
    hub_sum_mask,
    hub_spread_mask,
    going,
    coming,
    hub_in,
    dense_out,
    dense_in,
    sums,
    pair,
    fix_pair,
    fixes,
    returning,
    returning_far,
    up_in,
    relay,
    returned,
    load_sem,
    map_sem,
    fetch_sem,
    ids_send,
    ids_recv,
    own_send,
    own_recv,
    hub_send,
    hub_recv,
    dense_send,
    dense_recv,
    pair_send,
    pair_recv,
    back_send,
    back_recv,
    up_send,
    up_recv,
    ret_send,
    relay_send,
    ret_recv,
):
    me = lax.axis_index("wide")
    side = lax.axis_index("narrow")
    comps, row_count, nodes = out.shape[1:]
    m = n // 2
    p = n // PLANES
    slots = m * capp
    blocks = sums.shape[1]
    half = blocks // 2
    upper = me // m
    local = lax.rem(me, m)
    line = lax.rem(me, p)
    base = upper * m
    far_base = (1 - upper) * m
    my_hubs = (1 + upper) * p
    far_hub = (2 - upper) * p + line
    is_hub = me // p == 1 + upper
    is_outer = jnp.logical_not(is_hub)
    my_plane = local // p
    far_planes = (1 - upper, upper)
    mine = pl.multiple_of(side * half, half)
    theirs = pl.multiple_of((1 - side) * half, half)

    if capp > cap:
        first_pad = cap // SUBLANES * SUBLANES
        pad = pl.ds(first_pad, capp - first_pad)
        empty = jnp.zeros((comps, m, capp - first_pad, nodes), jnp.float32)
        coming[:, :, pad, :] = empty
        hub_in[:, 0, :, pad, :] = empty
        hub_in[:, 1, :, pad, :] = empty
        returned[:, 0:m, pad, :] = empty
        returned[:, m:n, pad, :] = empty

    barrier = pltpu.get_barrier_semaphore()

    def greet(device):
        pl.semaphore_signal(barrier, inc=1, device_id=device, device_id_type=MESH)

    def greet_half(k, carry):
        greet({"wide": base + lax.rem(local + k, m)})
        return carry

    lax.fori_loop(1, m, greet_half, 0)
    greet({"narrow": 1 - side})
    for s in range(2):
        greet({"wide": far_hub, "narrow": s})

    @pl.when(is_hub)
    def _():
        for s in range(2):
            for j in range(2):
                greet({"wide": far_base + j * p + line, "narrow": s})

    map_loads = [
        pltpu.make_async_copy(send_hbm, send_map, map_sem.at[0]),
        pltpu.make_async_copy(arrival_hbm, arrival_map, map_sem.at[1]),
    ]
    loads = [
        pltpu.make_async_copy(contributions_hbm.at[0, c], contributions.at[c], load_sem.at[c])
        for c in range(comps)
    ]
    fetches = [
        pltpu.make_async_copy(diagonal_hbm.at[pl.ds(mine, half)], diagonal, fetch_sem.at[0]),
        pltpu.make_async_copy(mortar_hbm.at[pl.ds(mine, half)], mortar, fetch_sem.at[1]),
        pltpu.make_async_copy(inverse_hbm.at[pl.ds(mine, half)], inverse, fetch_sem.at[2]),
    ]
    for copy in map_loads + loads:
        copy.start()

    def stretch(target, first, source, count):
        target[...] = jnp.full(target.shape, -1, jnp.int32)
        for k in range(count):
            ids = source[0:1, (first + k) * cap : (first + k + 1) * cap]
            target[:, k * capp : k * capp + cap] = jnp.broadcast_to(ids, (SUBLANES, cap))

    def row_mask(ids, count):
        shape = (count // SUBLANES, SUBLANES, ids.shape[1])
        rows = lax.broadcasted_iota(jnp.int32, shape, 0) * SUBLANES + lax.broadcasted_iota(
            jnp.int32, shape, 1
        )
        hits = jnp.where(ids[None] == rows, 1.0, 0.0)
        return hits.reshape(count, ids.shape[1]).astype(jnp.bfloat16)

    def column_mask(target, ids):
        lanes = lax.broadcasted_iota(jnp.int32, (LANES, LANES), 1)
        for k in range(target.shape[0] // LANES):
            row = ids[0:1, k * LANES : (k + 1) * LANES]
            column = jnp.broadcast_to(row, (LANES, LANES)).T
            for g in range(target.shape[1] // LANES):
                hits = jnp.where(column == lanes + g * LANES, 1.0, 0.0)
                target[k * LANES : (k + 1) * LANES, g * LANES : (g + 1) * LANES] = hits.astype(
                    jnp.bfloat16
                )

    def wait_bytes(view, sem):
        with jax.named_scope("wait"):
            pltpu.make_async_copy(view, view, sem).wait()

    def remote(source, target, send_sem, recv_sem, device):
        return pltpu.make_async_remote_copy(
            src_ref=source,
            dst_ref=target,
            send_sem=send_sem,
            recv_sem=recv_sem,
            device_id=device,
            device_id_type=MESH,
        )

    live = pl.ds(0, cap)
    straight_back = (0,1,2)

    def back_planes(c):
        return far_planes[:1] if c in straight_back else far_planes

    def each_peer(send):
        def cross(k, carry):
            send((1 - my_plane) * p + lax.rem(line + k, p))
            return carry

        def along(k, carry):
            send(my_plane * p + lax.rem(line + k, p))
            return carry

        lax.fori_loop(0, p, cross, 0)
        lax.fori_loop(1, p, along, 0)

    def pick(c):
        with jax.named_scope(f"pick{c}"):
            loads[c].wait()
            going[c] = one_hot_dot(pick_mask[...], contributions[c]).reshape(n, capp, nodes)

    def send_hub(c):
        with jax.named_scope(f"send_hub{c}"):
            for j in far_planes:

                def to_hub(k, carry):
                    other = lax.rem(line + k, p)
                    remote(
                        going.at[c, far_base + j * p + other, live],
                        hub_in.at[c, j, local, live],
                        hub_send.at[c],
                        hub_recv.at[c, j],
                        {"wide": my_hubs + other},
                    ).start()
                    return carry

                @pl.when(is_outer)
                def _():
                    to_hub(0, 0)

                lax.fori_loop(1, p, to_hub, 0)

            @pl.when(is_hub)
            def _():
                for j in range(2):
                    hub_in[c, j, local] = going[c, far_base + j * p + line]

    def send_own(c):
        with jax.named_scope(f"send_own{c}"):

            def to_owner(peer):
                remote(
                    going.at[c, base + peer, live],
                    coming.at[c, local, live],
                    own_send.at[c],
                    own_recv.at[c],
                    {"wide": base + peer},
                ).start()

            each_peer(to_owner)
            coming[c, local] = going[c, me]

    def gather_hub(c):
        with jax.named_scope(f"gather_hub{c}"):
            @pl.when(is_hub)
            def _():
                for j in far_planes:
                    wait_bytes(hub_in.at[c, j, pl.ds(0, m - 1), live], hub_recv.at[c, j])
                    dense_out[c, j] = one_hot_dot(
                        hub_sum_mask[j], hub_in[c, j].reshape(slots, nodes)
                    )
                    for s in range(2):
                        remote(
                            dense_out.at[c, j, pl.ds(s * half, half)],
                            dense_in.at[c, side],
                            dense_send.at[c, j],
                            dense_recv.at[c],
                            {"wide": far_base + j * p + line, "narrow": s},
                        ).start()

    def swap(c):
        return remote(
            sums.at[c, pl.ds(theirs, half)],
            pair.at[c, side],
            pair_send.at[c],
            pair_recv.at[c],
            {"narrow": 1 - side},
        )

    def gather_own(c):
        with jax.named_scope(f"gather_own{c}"):
            wait_bytes(coming.at[c, pl.ds(0, m - 1), live], own_recv.at[c])
            sums[c] = one_hot_dot(sum_mask[...], coming[c].reshape(slots, nodes))
            swap(c).start()
            pair[c, side] = sums[c, pl.ds(mine, half), :]

    def swap_back(c):
        return remote(
            fix_pair.at[c, 1 - side],
            fixes.at[c, pl.ds(mine, half)],
            back_send.at[c],
            back_recv.at[c],
            {"narrow": 1 - side},
        )

    def raise_fixes(c):
        def to_far_hub():
            for s in range(2):
                remote(
                    fix_pair.at[c, s],
                    up_in.at[c, my_plane, pl.ds(mine, half)],
                    up_send.at[c],
                    up_recv.at[c, my_plane],
                    {"wide": far_hub, "narrow": s},
                ).start()

        if c in straight_back:
            pl.when(is_outer)(to_far_hub)
        else:
            to_far_hub()

    def await_sums(c):
        with jax.named_scope(f"await_sums{c}"):
            with jax.named_scope("wait_swap"):
                swap(c).wait()
            wait_bytes(dense_in.at[c], dense_recv.at[c])

    def solve(c):
        with jax.named_scope(f"solve{c}"):

            def condense(g, carry):
                first = pl.multiple_of(g * GROUP, GROUP)
                rows = pl.ds(first, GROUP)
                slave = pair[c, 0, rows, :] + dense_in[c, 0, rows, :]
                master = pair[c, 1, rows, :] + dense_in[c, 1, rows, :]
                scale = diagonal[rows, :]
                condensed = master + block_products(slave / scale, lambda b: mortar[first + b], False)
                master_fix = block_products(condensed, lambda b: inverse[first + b], True)
                slave_fix = block_products(master_fix, lambda b: mortar[first + b], True) / scale
                fix_pair[c, 0, rows, :] = slave_fix
                fix_pair[c, 1, rows, :] = master_fix
                return carry

            lax.fori_loop(0, half // GROUP, condense, 0, unroll=2)
            swap_back(c).start()
            fixes[c, pl.ds(mine, half), :] = fix_pair[c, side]

    def return_own(c):
        with jax.named_scope(f"return_own{c}"):
            with jax.named_scope("wait_back"):
                swap_back(c).wait()
            if c in straight_back:

                @pl.when(is_hub)
                def _():
                    returning_far[c] = one_hot_dot(far_spread_mask[...], fixes[c]).reshape(
                        m, capp, nodes
                    )

                    def to_far(k, carry):
                        peer = lax.rem(local + k, m)
                        remote(
                            returning_far.at[c, peer, live],
                            returned.at[c, me, live],
                            ret_send.at[c],
                            ret_recv.at[c],
                            {"wide": far_base + peer},
                        ).start()
                        return carry

                    lax.fori_loop(0, m, to_far, 0)

            returning[c] = one_hot_dot(spread_mask[...], fixes[c]).reshape(m, capp, nodes)

            def to_source(peer):
                remote(
                    returning.at[c, peer, live],
                    returned.at[c, me, live],
                    ret_send.at[c],
                    ret_recv.at[c],
                    {"wide": base + peer},
                ).start()

            each_peer(to_source)
            returned[c, me] = returning[c, local]

    def return_hub(c):
        @pl.when(is_hub)
        def _():
            with jax.named_scope(f"return_hub{c}"):
                for j in back_planes(c):
                    owner = far_base + j * p + line
                    wait_bytes(up_in.at[c, j], up_recv.at[c, j])
                    relay[c, j] = one_hot_dot(hub_spread_mask[j], up_in[c, j]).reshape(
                        m, capp, nodes
                    )

                    def to_source(peer):
                        remote(
                            relay.at[c, j, peer, live],
                            returned.at[c, owner, live],
                            relay_send.at[c, j],
                            ret_recv.at[c],
                            {"wide": base + peer},
                        ).start()

                    each_peer(to_source)
                    returned[c, owner] = relay[c, j, local]

    def place(c):
        with jax.named_scope(f"place{c}"):
            at_hub = len(back_planes(c))

            @pl.when(is_hub)
            def _():
                wait_bytes(returned.at[c, pl.ds(0, n - 1 - at_hub), live], ret_recv.at[c])

            @pl.when(is_outer)
            def _():
                wait_bytes(returned.at[c, pl.ds(0, n - 1), live], ret_recv.at[c])

            out[0, c] = one_hot_dot(place_mask[...], returned[c].reshape(n * capp, nodes))

    map_loads[0].wait()
    with jax.named_scope("pick_mask"):
        stretch(send_row, 0, send_map, n)
        column_mask(pick_mask, send_row)
    map_loads[1].wait()

    pick(0)
    for fetch in fetches:
        fetch.start()
    with jax.named_scope("rows"):

        @pl.when(upper == 0)
        def _():
            stretch(own_row, 0, arrival_map, m)
            stretch(far_row, m, arrival_map, m)

        @pl.when(upper == 1)
        def _():
            stretch(far_row, 0, arrival_map, m)
            stretch(own_row, m, arrival_map, m)

    with jax.named_scope("entry"):
        pl.semaphore_wait(barrier, jnp.where(is_hub, m + 6, m + 2))
    send_ids = remote(
        far_row,
        hub_rows.at[my_plane],
        ids_send.at[0],
        ids_recv.at[my_plane],
        {"wide": far_hub},
    )
    send_ids.start()
    send_hub(0)
    pick(1)
    send_hub(1)
    send_own(0)
    pick(2)
    send_hub(2)
    send_own(1)
    send_own(2)
    with jax.named_scope("own_masks"):
        sum_mask[...] = row_mask(own_row[...], blocks)
        column_mask(spread_mask, own_row)

    @pl.when(is_hub)
    def _():
        with jax.named_scope("hub_masks"):
            column_mask(far_spread_mask, far_row)
            for j in far_planes:
                wait_bytes(hub_rows.at[j], ids_recv.at[j])
                hub_sum_mask[j] = row_mask(hub_rows[j], blocks)
                column_mask(hub_spread_mask.at[j], hub_rows.at[j])

    gather_hub(0)
    with jax.named_scope("place_mask"):
        place_mask[...] = row_mask(send_row[...], row_count)
    gather_hub(1)
    gather_own(0)
    for fetch in fetches:
        fetch.wait()
    gather_hub(2)
    await_sums(0)
    solve(0)
    raise_fixes(0)
    gather_own(1)
    return_own(0)
    await_sums(1)
    solve(1)
    return_hub(0)
    gather_own(2)
    return_own(1)
    await_sums(2)
    raise_fixes(1)
    solve(2)
    raise_fixes(2)
    return_hub(1)
    return_own(2)
    return_hub(2)
    place(0)
    place(1)
    place(2)

    with jax.named_scope("drain"):
        send_ids.wait_send()
        for c in range(comps):
            wait_bytes(going.at[c, pl.ds(0, m - 1), live], own_send.at[c])

            @pl.when(is_hub)
            def _():
                wait_bytes(going.at[c, pl.ds(0, m - 2), live], hub_send.at[c])
                for j in range(2):
                    wait_bytes(dense_out.at[c, j], dense_send.at[c, j])
                for j in back_planes(c):
                    wait_bytes(relay.at[c, j, pl.ds(0, m - 1), live], relay_send.at[c, j])
                if c in straight_back:
                    wait_bytes(going.at[c, pl.ds(0, n - 1), live], ret_send.at[c])
                else:
                    wait_bytes(going.at[c, pl.ds(0, m - 1), live], ret_send.at[c])
                    wait_bytes(fix_pair.at[c], up_send.at[c])

            @pl.when(is_outer)
            def _():
                wait_bytes(going.at[c, pl.ds(0, m), live], hub_send.at[c])
                wait_bytes(going.at[c, pl.ds(0, m - 1), live], ret_send.at[c])
                wait_bytes(fix_pair.at[c], up_send.at[c])


def shards(contributions, send_map, arrival_map, dual_diagonal, mortar, master_inverse):
    n = lax.axis_size("wide")
    _, comps, row_count, nodes = contributions.shape
    blocks = dual_diagonal.shape[0]
    half = blocks // lax.axis_size("narrow")
    m = n // 2
    cap = send_map.shape[1] // n
    capp = -(-cap // SUBLANES) * SUBLANES
    while m * capp % LANES:
        capp += SUBLANES
    slots = m * capp

    operands = tuple(
        pltpu.with_memory_space_constraint(x, pltpu.HBM)
        for x in (contributions, send_map, arrival_map, dual_diagonal, mortar, master_inverse)
    )
    f32, bf16, i32 = jnp.float32, jnp.bfloat16, jnp.int32
    dma = pltpu.SemaphoreType.DMA
    return pl.pallas_call(
        functools.partial(kernel, n, cap, capp),
        out_shape=jax.ShapeDtypeStruct((1, comps, row_count, nodes), f32),
        in_specs=[pl.BlockSpec(memory_space=pltpu.HBM)] * 6,
        out_specs=pl.BlockSpec(memory_space=pltpu.VMEM),
        scratch_shapes=[
            pltpu.VMEM((comps, row_count, nodes), f32),
            pltpu.VMEM((1, n * cap), i32),
            pltpu.VMEM((1, n * cap), i32),
            pltpu.VMEM((half, nodes), f32),
            pltpu.VMEM((half, nodes, nodes), bf16),
            pltpu.VMEM((half, nodes, nodes), bf16),
            pltpu.VMEM((SUBLANES, n * capp), i32),
            pltpu.VMEM((SUBLANES, slots), i32),
            pltpu.VMEM((SUBLANES, slots), i32),
            pltpu.VMEM((2, SUBLANES, slots), i32),
            pltpu.VMEM((n * capp, row_count), bf16),
            pltpu.VMEM((row_count, n * capp), bf16),
            pltpu.VMEM((blocks, slots), bf16),
            pltpu.VMEM((slots, blocks), bf16),
            pltpu.VMEM((slots, blocks), bf16),
            pltpu.VMEM((2, blocks, slots), bf16),
            pltpu.VMEM((2, slots, blocks), bf16),
            pltpu.VMEM((comps, n, capp, nodes), f32),
            pltpu.VMEM((comps, m, capp, nodes), f32),
            pltpu.VMEM((comps, 2, m, capp, nodes), f32),
            pltpu.VMEM((comps, 2, blocks, nodes), f32),
            pltpu.VMEM((comps, 2, half, nodes), f32),
            pltpu.VMEM((comps, blocks, nodes), f32),
            pltpu.VMEM((comps, 2, half, nodes), f32),
            pltpu.VMEM((comps, 2, half, nodes), f32),
            pltpu.VMEM((comps, blocks, nodes), f32),
            pltpu.VMEM((comps, m, capp, nodes), f32),
            pltpu.VMEM((comps, m, capp, nodes), f32),
            pltpu.VMEM((comps, 2, blocks, nodes), f32),
            pltpu.VMEM((comps, 2, m, capp, nodes), f32),
            pltpu.VMEM((comps, n, capp, nodes), f32),
            dma((comps,)),
            dma((2,)),
            dma((3,)),
            dma((1,)),
            dma((2,)),
            dma((comps,)),
            dma((comps,)),
            dma((comps,)),
            dma((comps, 2)),
            dma((comps, 2)),
            dma((comps,)),
            dma((comps,)),
            dma((comps,)),
            dma((comps,)),
            dma((comps,)),
            dma((comps,)),
            dma((comps, 2)),
            dma((comps,)),
            dma((comps, 2)),
            dma((comps,)),
        ],
        compiler_params=pltpu.CompilerParams(
            collective_id=0, has_side_effects=True, vmem_limit_bytes=48 * 1024 * 1024
        ),
    )(*operands)


def solution(mesh):
    placed = (
        P("narrow", None, "wide", None),
        P("wide", None),
        P("wide", None),
        P("wide", None),
        P("wide", None, None),
        P("wide", None, None),
    )
    return jax.shard_map(
        shards,
        mesh=mesh,
        in_specs=placed,
        out_specs=P("narrow", None, "wide", None),
        check_vma=False,
    )
```

```python
import functools

import jax
import jax.numpy as jnp
from jax import lax
from jax.experimental import pallas as pl
from jax.experimental.pallas import tpu as pltpu
from jax.sharding import PartitionSpec as P

GROUP = 32
SUBLANES = 8
LANES = 128
PLANES = 4
MESH = pl.DeviceIdType.MESH


def one_hot_dot(mask, values):
    nodes = values.shape[1]
    high = values.astype(jnp.bfloat16)
    low = (values - high.astype(jnp.float32)).astype(jnp.bfloat16)
    both = jnp.dot(mask, jnp.concatenate([high, low], axis=1), preferred_element_type=jnp.float32)
    return both[:, :nodes] + both[:, nodes:]


def block_products(vectors, matrices, transposed):
    nodes = vectors.shape[1]
    rows = lax.broadcasted_iota(jnp.int32, vectors.shape, 0)
    odd = lax.rem(rows, 2) == 1
    total = jnp.zeros(vectors.shape, jnp.float32)
    wide = jnp.concatenate(
        [jnp.where(odd, total, vectors), jnp.where(odd, vectors, total)], axis=1
    ).astype(jnp.bfloat16)
    for b in range(0, vectors.shape[0], 4):
        m0, m1, m2, m3 = (matrices(b + k) for k in range(4))
        if transposed:
            tile = [[m0, m1], [m2, m3]]
        else:
            tile = [[m0, m2], [m1, m3]]
        tile = jnp.concatenate([jnp.concatenate(part, axis=1) for part in tile], axis=0)
        product = lax.dot_general(
            wide,
            tile,
            (((1,), (1 if transposed else 0,)), ((), ())),
            preferred_element_type=jnp.float32,
        )
        first = (rows >= b) & (rows < b + 2)
        second = (rows >= b + 2) & (rows < b + 4)
        total = jnp.where(first, product[:, :nodes], jnp.where(second, product[:, nodes:], total))
    return total


def kernel(
    n,
    cap,
    capp,
    contributions_hbm,
    send_hbm,
    arrival_hbm,
    diagonal_hbm,
    mortar_hbm,
    inverse_hbm,
    out,
    contributions,
    send_map,
    arrival_map,
    diagonal,
    mortar,
    inverse,
    send_row,
    own_row,
    far_row,
    hub_rows,
    pick_mask,
    place_mask,
    sum_mask,
    spread_mask,
    far_spread_mask,
    hub_sum_mask,
    hub_spread_mask,
    going,
    coming,
    hub_in,
    dense_out,
    dense_in,
    sums,
    pair,
    fix_pair,
    fixes,
    returning,
    returning_far,
    up_in,
    relay,
    returned,
    load_sem,
    map_sem,
    fetch_sem,
    ids_send,
    ids_recv,
    own_send,
    own_recv,
    hub_send,
    hub_recv,
    dense_send,
    dense_recv,
    pair_send,
    pair_recv,
    back_send,
    back_recv,
    up_send,
    up_recv,
    ret_send,
    relay_send,
    ret_recv,
    far_recv,
):
    me = lax.axis_index("wide")
    side = lax.axis_index("narrow")
    comps, row_count, nodes = out.shape[1:]
    m = n // 2
    p = n // PLANES
    slots = m * capp
    blocks = sums.shape[1]
    half = blocks // 2
    upper = me // m
    local = lax.rem(me, m)
    line = lax.rem(me, p)
    base = upper * m
    far_base = (1 - upper) * m
    my_hubs = (1 + upper) * p
    far_hub = (2 - upper) * p + line
    is_hub = me // p == 1 + upper
    is_outer = jnp.logical_not(is_hub)
    my_plane = local // p
    far_planes = (1 - upper, upper)
    mine = pl.multiple_of(side * half, half)
    theirs = pl.multiple_of((1 - side) * half, half)

    if capp > cap:
        first_pad = cap // SUBLANES * SUBLANES
        pad = pl.ds(first_pad, capp - first_pad)
        empty = jnp.zeros((comps, m, capp - first_pad, nodes), jnp.float32)
        coming[:, :, pad, :] = empty
        hub_in[:, 0, :, pad, :] = empty
        hub_in[:, 1, :, pad, :] = empty
        returned[:, 0:m, pad, :] = empty
        returned[:, m:n, pad, :] = empty

    barrier = pltpu.get_barrier_semaphore()

    def greet(device):
        pl.semaphore_signal(barrier, inc=1, device_id=device, device_id_type=MESH)

    def greet_half(k, carry):
        greet({"wide": base + lax.rem(local + k, m)})
        return carry

    lax.fori_loop(1, m, greet_half, 0)
    greet({"narrow": 1 - side})
    for s in range(2):
        greet({"wide": far_hub, "narrow": s})

    @pl.when(is_hub)
    def _():
        for s in range(2):
            for j in range(2):
                greet({"wide": far_base + j * p + line, "narrow": s})

    map_loads = [
        pltpu.make_async_copy(send_hbm, send_map, map_sem.at[0]),
        pltpu.make_async_copy(arrival_hbm, arrival_map, map_sem.at[1]),
    ]
    loads = [
        pltpu.make_async_copy(contributions_hbm.at[0, c], contributions.at[c], load_sem.at[c])
        for c in range(comps)
    ]
    fetches = [
        pltpu.make_async_copy(diagonal_hbm.at[pl.ds(mine, half)], diagonal, fetch_sem.at[0]),
        pltpu.make_async_copy(mortar_hbm.at[pl.ds(mine, half)], mortar, fetch_sem.at[1]),
        pltpu.make_async_copy(inverse_hbm.at[pl.ds(mine, half)], inverse, fetch_sem.at[2]),
    ]
    for copy in map_loads + loads:
        copy.start()

    def stretch(target, first, source, count):
        target[...] = jnp.full(target.shape, -1, jnp.int32)
        for k in range(count):
            ids = source[0:1, (first + k) * cap : (first + k + 1) * cap]
            target[:, k * capp : k * capp + cap] = jnp.broadcast_to(ids, (SUBLANES, cap))

    def row_mask(ids, count):
        shape = (count // SUBLANES, SUBLANES, ids.shape[1])
        rows = lax.broadcasted_iota(jnp.int32, shape, 0) * SUBLANES + lax.broadcasted_iota(
            jnp.int32, shape, 1
        )
        hits = jnp.where(ids[None] == rows, 1.0, 0.0)
        return hits.reshape(count, ids.shape[1]).astype(jnp.bfloat16)

    def column_mask(target, ids):
        lanes = lax.broadcasted_iota(jnp.int32, (LANES, LANES), 1)
        for k in range(target.shape[0] // LANES):
            row = ids[0:1, k * LANES : (k + 1) * LANES]
            column = jnp.broadcast_to(row, (LANES, LANES)).T
            for g in range(target.shape[1] // LANES):
                hits = jnp.where(column == lanes + g * LANES, 1.0, 0.0)
                target[k * LANES : (k + 1) * LANES, g * LANES : (g + 1) * LANES] = hits.astype(
                    jnp.bfloat16
                )

    def wait_bytes(view, sem):
        with jax.named_scope("wait"):
            pltpu.make_async_copy(view, view, sem).wait()

    def remote(source, target, send_sem, recv_sem, device):
        return pltpu.make_async_remote_copy(
            src_ref=source,
            dst_ref=target,
            send_sem=send_sem,
            recv_sem=recv_sem,
            device_id=device,
            device_id_type=MESH,
        )

    live = pl.ds(0, cap)
    straight_back = (0,1,2)

    def back_planes(c):
        return far_planes[:1] if c in straight_back else far_planes

    def each_peer(send):
        def cross(k, carry):
            send((1 - my_plane) * p + lax.rem(line + k, p))
            return carry

        def along(k, carry):
            send(my_plane * p + lax.rem(line + k, p))
            return carry

        lax.fori_loop(0, p, cross, 0)
        lax.fori_loop(1, p, along, 0)

    def pick(c):
        with jax.named_scope(f"pick{c}"):
            loads[c].wait()
            going[c] = one_hot_dot(pick_mask[...], contributions[c]).reshape(n, capp, nodes)

    def send_hub(c):
        with jax.named_scope(f"send_hub{c}"):
            for j in far_planes:

                def to_hub(k, carry):
                    other = lax.rem(line + k, p)
                    remote(
                        going.at[c, far_base + j * p + other, live],
                        hub_in.at[c, j, local, live],
                        hub_send.at[c],
                        hub_recv.at[c, j],
                        {"wide": my_hubs + other},
                    ).start()
                    return carry

                @pl.when(is_outer)
                def _():
                    to_hub(0, 0)

                lax.fori_loop(1, p, to_hub, 0)

            @pl.when(is_hub)
            def _():
                for j in range(2):
                    hub_in[c, j, local] = going[c, far_base + j * p + line]

    def send_own(c):
        with jax.named_scope(f"send_own{c}"):

            def to_owner(peer):
                remote(
                    going.at[c, base + peer, live],
                    coming.at[c, local, live],
                    own_send.at[c],
                    own_recv.at[c],
                    {"wide": base + peer},
                ).start()

            each_peer(to_owner)
            coming[c, local] = going[c, me]

    def gather_hub(c):
        with jax.named_scope(f"gather_hub{c}"):
            @pl.when(is_hub)
            def _():
                for j in far_planes:
                    wait_bytes(hub_in.at[c, j, pl.ds(0, m - 1), live], hub_recv.at[c, j])
                    dense_out[c, j] = one_hot_dot(
                        hub_sum_mask[j], hub_in[c, j].reshape(slots, nodes)
                    )
                    for s in range(2):
                        remote(
                            dense_out.at[c, j, pl.ds(s * half, half)],
                            dense_in.at[c, side],
                            dense_send.at[c, j],
                            dense_recv.at[c],
                            {"wide": far_base + j * p + line, "narrow": s},
                        ).start()

    def swap(c):
        return remote(
            sums.at[c, pl.ds(theirs, half)],
            pair.at[c, side],
            pair_send.at[c],
            pair_recv.at[c],
            {"narrow": 1 - side},
        )

    def gather_own(c):
        with jax.named_scope(f"gather_own{c}"):
            wait_bytes(coming.at[c, pl.ds(0, m - 1), live], own_recv.at[c])
            sums[c] = one_hot_dot(sum_mask[...], coming[c].reshape(slots, nodes))
            swap(c).start()
            pair[c, side] = sums[c, pl.ds(mine, half), :]

    def swap_back(c):
        return remote(
            fix_pair.at[c, 1 - side],
            fixes.at[c, pl.ds(mine, half)],
            back_send.at[c],
            back_recv.at[c],
            {"narrow": 1 - side},
        )

    def raise_fixes(c):
        def to_far_hub():
            for s in range(2):
                remote(
                    fix_pair.at[c, s],
                    up_in.at[c, my_plane, pl.ds(mine, half)],
                    up_send.at[c],
                    up_recv.at[c, my_plane],
                    {"wide": far_hub, "narrow": s},
                ).start()

        if c in straight_back:
            pl.when(is_outer)(to_far_hub)
        else:
            to_far_hub()

    def await_sums(c):
        with jax.named_scope(f"await_sums{c}"):
            with jax.named_scope("wait_swap"):
                swap(c).wait()
            wait_bytes(dense_in.at[c], dense_recv.at[c])

    def solve(c):
        with jax.named_scope(f"solve{c}"):

            def condense(g, carry):
                first = pl.multiple_of(g * GROUP, GROUP)
                rows = pl.ds(first, GROUP)
                slave = pair[c, 0, rows, :] + dense_in[c, 0, rows, :]
                master = pair[c, 1, rows, :] + dense_in[c, 1, rows, :]
                scale = diagonal[rows, :]
                condensed = master + block_products(slave / scale, lambda b: mortar[first + b], False)
                master_fix = block_products(condensed, lambda b: inverse[first + b], True)
                slave_fix = block_products(master_fix, lambda b: mortar[first + b], True) / scale
                fix_pair[c, 0, rows, :] = slave_fix
                fix_pair[c, 1, rows, :] = master_fix
                return carry

            lax.fori_loop(0, half // GROUP, condense, 0, unroll=2)
            swap_back(c).start()
            fixes[c, pl.ds(mine, half), :] = fix_pair[c, side]

    def return_own(c):
        with jax.named_scope(f"return_own{c}"):
            with jax.named_scope("wait_back"):
                swap_back(c).wait()
            if c in straight_back:

                @pl.when(is_hub)
                def _():
                    returning_far[c] = one_hot_dot(far_spread_mask[...], fixes[c]).reshape(
                        m, capp, nodes
                    )

                    def to_far(k, carry):
                        peer = lax.rem(local + k, m)
                        remote(
                            returning_far.at[c, peer, live],
                            returned.at[c, me, live],
                            ret_send.at[c],
                            far_recv.at[c],
                            {"wide": far_base + peer},
                        ).start()
                        return carry

                    lax.fori_loop(0, m, to_far, 0)

            returning[c] = one_hot_dot(spread_mask[...], fixes[c]).reshape(m, capp, nodes)

            def to_source(peer):
                remote(
                    returning.at[c, peer, live],
                    returned.at[c, me, live],
                    ret_send.at[c],
                    ret_recv.at[c],
                    {"wide": base + peer},
                ).start()

            each_peer(to_source)
            returned[c, me] = returning[c, local]

    def return_hub(c):
        @pl.when(is_hub)
        def _():
            with jax.named_scope(f"return_hub{c}"):
                for j in back_planes(c):
                    owner = far_base + j * p + line
                    wait_bytes(up_in.at[c, j], up_recv.at[c, j])
                    relay[c, j] = one_hot_dot(hub_spread_mask[j], up_in[c, j]).reshape(
                        m, capp, nodes
                    )

                    def to_source(peer):
                        remote(
                            relay.at[c, j, peer, live],
                            returned.at[c, owner, live],
                            relay_send.at[c, j],
                            far_recv.at[c],
                            {"wide": base + peer},
                        ).start()

                    each_peer(to_source)
                    returned[c, owner] = relay[c, j, local]

    def place(c):
        with jax.named_scope(f"place{c}"):
            at_hub = len(back_planes(c))

            def half_of(first):
                columns = pl.ds(pl.multiple_of(first * capp, LANES), slots)
                rows = returned[c, pl.ds(first, m)].reshape(slots, nodes)
                return one_hot_dot(place_mask[:, columns], rows)

            wait_bytes(returned.at[c, pl.ds(0, m - 1), live], ret_recv.at[c])
            out[0, c] = half_of(base)

            @pl.when(is_hub)
            def _():
                wait_bytes(returned.at[c, pl.ds(0, m - at_hub), live], far_recv.at[c])

            @pl.when(is_outer)
            def _():
                wait_bytes(returned.at[c, pl.ds(0, m), live], far_recv.at[c])

            out[0, c] += half_of(far_base)

    map_loads[0].wait()
    with jax.named_scope("pick_mask"):
        stretch(send_row, 0, send_map, n)
        column_mask(pick_mask, send_row)
    map_loads[1].wait()

    pick(0)
    for fetch in fetches:
        fetch.start()
    with jax.named_scope("rows"):

        @pl.when(upper == 0)
        def _():
            stretch(own_row, 0, arrival_map, m)
            stretch(far_row, m, arrival_map, m)

        @pl.when(upper == 1)
        def _():
            stretch(far_row, 0, arrival_map, m)
            stretch(own_row, m, arrival_map, m)

    with jax.named_scope("entry"):
        pl.semaphore_wait(barrier, jnp.where(is_hub, m + 6, m + 2))
    send_ids = remote(
        far_row,
        hub_rows.at[my_plane],
        ids_send.at[0],
        ids_recv.at[my_plane],
        {"wide": far_hub},
    )
    send_ids.start()
    send_hub(0)
    pick(1)
    send_hub(1)
    send_own(0)
    pick(2)
    send_hub(2)
    send_own(1)
    send_own(2)
    with jax.named_scope("own_masks"):
        sum_mask[...] = row_mask(own_row[...], blocks)
        column_mask(spread_mask, own_row)

    @pl.when(is_hub)
    def _():
        with jax.named_scope("hub_masks"):
            column_mask(far_spread_mask, far_row)
            for j in far_planes:
                wait_bytes(hub_rows.at[j], ids_recv.at[j])
                hub_sum_mask[j] = row_mask(hub_rows[j], blocks)
                column_mask(hub_spread_mask.at[j], hub_rows.at[j])

    gather_hub(0)
    with jax.named_scope("place_mask"):
        place_mask[...] = row_mask(send_row[...], row_count)
    gather_hub(1)
    gather_own(0)
    for fetch in fetches:
        fetch.wait()
    gather_hub(2)
    await_sums(0)
    solve(0)
    raise_fixes(0)
    gather_own(1)
    return_own(0)
    await_sums(1)
    solve(1)
    return_hub(0)
    gather_own(2)
    return_own(1)
    await_sums(2)
    raise_fixes(1)
    solve(2)
    raise_fixes(2)
    return_hub(1)
    return_own(2)
    return_hub(2)
    place(0)
    place(1)
    place(2)

    with jax.named_scope("drain"):
        send_ids.wait_send()
        for c in range(comps):
            wait_bytes(going.at[c, pl.ds(0, m - 1), live], own_send.at[c])

            @pl.when(is_hub)
            def _():
                wait_bytes(going.at[c, pl.ds(0, m - 2), live], hub_send.at[c])
                for j in range(2):
                    wait_bytes(dense_out.at[c, j], dense_send.at[c, j])
                for j in back_planes(c):
                    wait_bytes(relay.at[c, j, pl.ds(0, m - 1), live], relay_send.at[c, j])
                if c in straight_back:
                    wait_bytes(going.at[c, pl.ds(0, n - 1), live], ret_send.at[c])
                else:
                    wait_bytes(going.at[c, pl.ds(0, m - 1), live], ret_send.at[c])
                    wait_bytes(fix_pair.at[c], up_send.at[c])

            @pl.when(is_outer)
            def _():
                wait_bytes(going.at[c, pl.ds(0, m), live], hub_send.at[c])
                wait_bytes(going.at[c, pl.ds(0, m - 1), live], ret_send.at[c])
                wait_bytes(fix_pair.at[c], up_send.at[c])


def shards(contributions, send_map, arrival_map, dual_diagonal, mortar, master_inverse):
    n = lax.axis_size("wide")
    _, comps, row_count, nodes = contributions.shape
    blocks = dual_diagonal.shape[0]
    half = blocks // lax.axis_size("narrow")
    m = n // 2
    cap = send_map.shape[1] // n
    capp = -(-cap // SUBLANES) * SUBLANES
    while m * capp % LANES:
        capp += SUBLANES
    slots = m * capp

    operands = tuple(
        pltpu.with_memory_space_constraint(x, pltpu.HBM)
        for x in (contributions, send_map, arrival_map, dual_diagonal, mortar, master_inverse)
    )
    f32, bf16, i32 = jnp.float32, jnp.bfloat16, jnp.int32
    dma = pltpu.SemaphoreType.DMA
    return pl.pallas_call(
        functools.partial(kernel, n, cap, capp),
        out_shape=jax.ShapeDtypeStruct((1, comps, row_count, nodes), f32),
        in_specs=[pl.BlockSpec(memory_space=pltpu.HBM)] * 6,
        out_specs=pl.BlockSpec(memory_space=pltpu.VMEM),
        scratch_shapes=[
            pltpu.VMEM((comps, row_count, nodes), f32),
            pltpu.VMEM((1, n * cap), i32),
            pltpu.VMEM((1, n * cap), i32),
            pltpu.VMEM((half, nodes), f32),
            pltpu.VMEM((half, nodes, nodes), bf16),
            pltpu.VMEM((half, nodes, nodes), bf16),
            pltpu.VMEM((SUBLANES, n * capp), i32),
            pltpu.VMEM((SUBLANES, slots), i32),
            pltpu.VMEM((SUBLANES, slots), i32),
            pltpu.VMEM((2, SUBLANES, slots), i32),
            pltpu.VMEM((n * capp, row_count), bf16),
            pltpu.VMEM((row_count, n * capp), bf16),
            pltpu.VMEM((blocks, slots), bf16),
            pltpu.VMEM((slots, blocks), bf16),
            pltpu.VMEM((slots, blocks), bf16),
            pltpu.VMEM((2, blocks, slots), bf16),
            pltpu.VMEM((2, slots, blocks), bf16),
            pltpu.VMEM((comps, n, capp, nodes), f32),
            pltpu.VMEM((comps, m, capp, nodes), f32),
            pltpu.VMEM((comps, 2, m, capp, nodes), f32),
            pltpu.VMEM((comps, 2, blocks, nodes), f32),
            pltpu.VMEM((comps, 2, half, nodes), f32),
            pltpu.VMEM((comps, blocks, nodes), f32),
            pltpu.VMEM((comps, 2, half, nodes), f32),
            pltpu.VMEM((comps, 2, half, nodes), f32),
            pltpu.VMEM((comps, blocks, nodes), f32),
            pltpu.VMEM((comps, m, capp, nodes), f32),
            pltpu.VMEM((comps, m, capp, nodes), f32),
            pltpu.VMEM((comps, 2, blocks, nodes), f32),
            pltpu.VMEM((comps, 2, m, capp, nodes), f32),
            pltpu.VMEM((comps, n, capp, nodes), f32),
            dma((comps,)),
            dma((2,)),
            dma((3,)),
            dma((1,)),
            dma((2,)),
            dma((comps,)),
            dma((comps,)),
            dma((comps,)),
            dma((comps, 2)),
            dma((comps, 2)),
            dma((comps,)),
            dma((comps,)),
            dma((comps,)),
            dma((comps,)),
            dma((comps,)),
            dma((comps,)),
            dma((comps, 2)),
            dma((comps,)),
            dma((comps, 2)),
            dma((comps,)),
            dma((comps,)),
        ],
        compiler_params=pltpu.CompilerParams(
            collective_id=0, has_side_effects=True, vmem_limit_bytes=48 * 1024 * 1024
        ),
    )(*operands)


def solution(mesh):
    placed = (
        P("narrow", None, "wide", None),
        P("wide", None),
        P("wide", None),
        P("wide", None),
        P("wide", None, None),
        P("wide", None, None),
    )
    return jax.shard_map(
        shards,
        mesh=mesh,
        in_specs=placed,
        out_specs=P("narrow", None, "wide", None),
        check_vma=False,
    )
```
